32 devices in a mesh: batch: 16 (over z, y, x), strip: 2 (over core).
Axes of the slice: x: 2, y: 2, z: 4, core: 2. Of those that a mesh axis runs over, the one named last changes fastest.
Arguments:
- state_maps: bfloat16 [16, 32, 64, 256], P('batch', 'strip'), may hold values from -6 to 6
- goal_maps: bfloat16 [16, 32, 64, 256], P('batch', 'strip'), may hold values from -6 to 6
- conv_one: bfloat16 [3, 3, 256, 256], replicated, may hold values from -0.125 to 0.125
- conv_two: bfloat16 [3, 3, 256, 256], replicated, may hold values from -0.125 to 0.125
- state_proj: bfloat16 [256, 1024], replicated, may hold values from -0.375 to 0.375
- goal_proj: bfloat16 [256, 1024], replicated, may hold values from -0.375 to 0.375
- inv_temp: float32 [1], replicated, may hold values from 4 to 16
- pair_index: int32 [16], P('batch'), may hold values from 0 to 15, each once
Outputs:
- pair_loss: float32 [16], P('batch')
- grad_state_proj: float32 [256, 1024], replicated
- grad_goal_proj: float32 [256, 1024], replicated
- block_maps: float32 [2, 16, 32, 64, 256], P(None, 'batch', 'strip')
The draws below stay inside these ranges and needn't reach their ends.
Inputs may be any that keep to these rules, and one draw needn't show every extreme that they name: pair_index names each goal of 0 to 15 exactly once.
All inputs are finite; a program needn't handle non-finite values.
Results may differ from the reference program's by a relative error of at most 0.017.
Values may be sent and summed in bfloat16 or wider, within the bound.
A program may use at most 64 MiB of HBM per device.

```python
import jax
import jax.numpy as jnp
from jax import lax

C = 256
E = 1024
COLS = 64
ROWS = 32
PAIRS = 16


def maps_draw(base_key):
    first_key, second_key = jax.random.split(base_key, 2)
    full_shape = (PAIRS, ROWS, COLS, C)
    rough_part = jax.random.normal(first_key, full_shape, jnp.float32)
    offset = jax.random.normal(second_key, (PAIRS, 1, 1, C), jnp.float32)
    return jnp.clip(0.7 * rough_part + offset, -6.0, 6.0).astype(jnp.bfloat16)


def draw_state_maps(key, part):
    return maps_draw(jax.random.fold_in(key, 11))


def draw_goal_maps(key, part):
    return maps_draw(jax.random.fold_in(key, 23))


def centred(own_key, extent, deviation, bound, kind=jnp.bfloat16):
    return jnp.clip(deviation * jax.random.normal(own_key, extent, jnp.float32), -bound, bound).astype(kind)


def setup_inputs(seed: int = 0) -> dict:
    keys = jax.random.split(jax.random.key(seed), 9)
    return {
        "state_maps": draw_state_maps(jax.random.fold_in(keys[8], 71), 0),
        "goal_maps": draw_goal_maps(jax.random.fold_in(keys[8], 71), 0),
        "conv_one": centred(keys[2], (3, 3, C, C), (9 * C) ** -0.5, 0.125),
        "conv_two": centred(keys[3], (3, 3, C, C), (9 * C) ** -0.5, 0.125),
        "state_proj": centred(keys[4], (C, E), C ** -0.5, 0.375),
        "goal_proj": centred(keys[5], (C, E), C ** -0.5, 0.375),
        "inv_temp": jnp.clip(jax.random.uniform(keys[6], (1,), jnp.float32, 4.0, 16.0), 4.0, 16.0),
        "pair_index": jax.random.permutation(keys[7], PAIRS).astype(jnp.int32),
    }


def conv_same(frame_maps, kernel):
    return lax.conv_general_dilated(frame_maps.astype(jnp.float32), kernel.astype(jnp.float32), (1, 1), ((1, 1), (1, 1)), dimension_numbers=('NHWC', 'HWIO', 'NHWC'), precision=lax.Precision.HIGHEST)

def encode(frame_maps, conv_one, conv_two):
    active = jnp.maximum(frame_maps, 0)
    first_out = jnp.maximum(conv_same(active, conv_one), 0.0).astype(jnp.bfloat16)
    block_out = jnp.maximum(frame_maps.astype(jnp.float32) + conv_same(first_out, conv_two), 0.0)
    return (lax.optimization_barrier(jnp.mean(block_out, axis=(1, 2))), block_out)

def pooled_all(frame_maps, conv_one, conv_two):
    grouped = frame_maps.reshape((PAIRS, 1) + frame_maps.shape[1:])
    pooled, block_out = lax.map(lambda block: encode(block, conv_one, conv_two), grouped)
    return (pooled.reshape(PAIRS, C), block_out.reshape(frame_maps.shape))

def normalize(embedding):
    inverse_norm = lax.rsqrt(lax.optimization_barrier(jnp.sum(embedding * embedding, axis=-1, keepdims=True)) + 1e-06)
    return (embedding * inverse_norm, inverse_norm)

def reference(state_maps, goal_maps, conv_one, conv_two, state_proj, goal_proj, inv_temp, pair_index):
    state_pooled, state_block = pooled_all(state_maps, conv_one, conv_two)
    goal_pooled, goal_block = pooled_all(goal_maps, conv_one, conv_two)
    block_maps = jnp.stack([state_block, goal_block], axis=0)
    state_pool = state_pooled.astype(jnp.bfloat16)
    goal_pool = goal_pooled.astype(jnp.bfloat16)
    state_emb = jnp.dot(state_pool, state_proj, preferred_element_type=jnp.float32)
    goal_emb = jnp.dot(goal_pool, goal_proj, preferred_element_type=jnp.float32)
    state_unit, state_inverse = normalize(state_emb)
    goal_unit, goal_inverse = normalize(goal_emb)
    state_bf = state_unit.astype(jnp.bfloat16)
    goal_bf = goal_unit.astype(jnp.bfloat16)
    sharpness = inv_temp[0]
    logits = sharpness * jnp.dot(state_bf, goal_bf.T, preferred_element_type=jnp.float32)
    exp_logits = jnp.exp(logits)
    row_total = lax.optimization_barrier(jnp.sum(exp_logits, axis=1))
    matched = jnp.arange(PAIRS, dtype=jnp.int32)[None, :] == pair_index[:, None]
    positive = lax.optimization_barrier(jnp.sum(jnp.where(matched, logits, 0.0), axis=1))
    pair_loss = jnp.log(row_total) - positive
    logit_grad = (exp_logits / row_total[:, None] - matched.astype(jnp.float32)).astype(jnp.bfloat16)
    state_unit_grad = sharpness * jnp.dot(logit_grad, goal_bf, preferred_element_type=jnp.float32)
    goal_unit_grad = sharpness * jnp.dot(logit_grad.T, state_bf, preferred_element_type=jnp.float32)
    state_emb_grad = ((state_unit_grad - state_unit * lax.optimization_barrier(jnp.sum(state_unit * state_unit_grad, axis=-1, keepdims=True))) * state_inverse).astype(jnp.bfloat16)
    goal_emb_grad = ((goal_unit_grad - goal_unit * lax.optimization_barrier(jnp.sum(goal_unit * goal_unit_grad, axis=-1, keepdims=True))) * goal_inverse).astype(jnp.bfloat16)
    grad_state_proj = jnp.dot(state_pool.T, state_emb_grad, preferred_element_type=jnp.float32)
    grad_goal_proj = jnp.dot(goal_pool.T, goal_emb_grad, preferred_element_type=jnp.float32)
    return (pair_loss, grad_state_proj, grad_goal_proj, block_maps)
```

```python
import functools

import jax
import jax.numpy as jnp
from jax import lax
from jax.experimental import pallas as pl
from jax.experimental.pallas import tpu as pltpu
from jax.sharding import PartitionSpec as P

MESH = pl.DeviceIdType.MESH
BF = jnp.bfloat16
F32 = jnp.float32
LANES = 128
ROWS_AT_ONCE = 6


def spread(dst, frame, row, cells):
    rows, columns, channels = cells.shape
    where = lax.broadcasted_iota(jnp.int32, cells.shape, 1)
    left = jnp.where(where == 0, 0.0, pltpu.roll(cells, 1, axis=1))
    right = jnp.where(where == columns - 1, 0.0, pltpu.roll(cells, columns - 1, axis=1))
    span = pl.ds(row, rows)
    dst[frame, span, :, 0:channels] = left.astype(BF)
    dst[frame, span, :, channels : 2 * channels] = cells.astype(BF)
    dst[frame, span, :, 2 * channels : 3 * channels] = right.astype(BF)


def chunks(start, stop):
    number = -(-(stop - start) // ROWS_AT_ONCE)
    cuts = [start + (stop - start) * i // number for i in range(number + 1)]
    return [(low, high - low) for low, high in zip(cuts, cuts[1:])]


def taps(src, frame, row, rows):
    columns, width = src.shape[2], src.shape[3]
    return jnp.concatenate(
        [src[frame, row + d : row + d + rows].reshape(rows * columns, width) for d in range(3)],
        axis=1,
    )


def block_kernel(
    batches, strips,
    state_ref, goal_ref, one_ref, two_ref, sproj_ref, gproj_ref, index_ref, temp_ref,
    block_ref, gathered_ref, sproj_out, gproj_out,
    maps, wide_one, wide_two, w_one, w_two, halo, index, temp, part, parts,
    load_sem, halo_send, halo_recv, part_send, part_recv,
):
    b = lax.axis_index("batch")
    s = lax.axis_index("strip")
    rows, columns, channels = maps.shape[1], maps.shape[2], maps.shape[3]
    packs = channels // LANES
    devices = batches * strips
    me = b * strips + s

    loads = [
        pltpu.make_async_copy(source, target, load_sem.at[i])
        for i, (source, target) in enumerate((
            (state_ref.at[0], maps.at[0]),
            (goal_ref.at[0], maps.at[1]),
            (one_ref, w_one),
            (two_ref, w_two),
            (sproj_ref, sproj_out),
            (gproj_ref, gproj_out),
            (index_ref, index),
            (temp_ref, temp),
        ))
    ]
    for copy in loads:
        copy.start()

    @pl.when(s == 0)
    def _():
        halo[0] = jnp.zeros(halo.shape[1:], BF)

    @pl.when(s == strips - 1)
    def _():
        halo[1] = jnp.zeros(halo.shape[1:], BF)

    barrier = pltpu.get_barrier_semaphore()

    def greet(k, carry):
        other = lax.rem(me + k, devices)
        pl.semaphore_signal(
            barrier, inc=1, device_id=(other // strips, lax.rem(other, strips)), device_id_type=MESH
        )
        return carry

    lax.fori_loop(1, devices, greet, 0)

    loads[0].wait()
    spread(wide_one, 0, 2, jnp.maximum(maps[0].astype(F32), 0.0))
    loads[1].wait()
    spread(wide_one, 1, 2, jnp.maximum(maps[1].astype(F32), 0.0))
    down = pltpu.make_async_remote_copy(
        src_ref=maps.at[:, rows - 2 : rows], dst_ref=halo.at[0],
        send_sem=halo_send.at[0], recv_sem=halo_recv.at[0],
        device_id=(b, lax.rem(s + 1, strips)), device_id_type=MESH,
    )
    up = pltpu.make_async_remote_copy(
        src_ref=maps.at[:, 0:2], dst_ref=halo.at[1],
        send_sem=halo_send.at[1], recv_sem=halo_recv.at[1],
        device_id=(b, lax.rem(s + strips - 1, strips)), device_id_type=MESH,
    )

    above = jnp.where(s > 0, 1.0, 0.0)
    below = jnp.where(s < strips - 1, 1.0, 0.0)

    def first(pieces):
        lhs = [taps(wide_one, f, r + 1, count) for f, r, count in pieces]
        lhs = lhs[0] if len(lhs) == 1 else jnp.concatenate(lhs, axis=0)
        out = jnp.maximum(jnp.dot(lhs, w_one[...], preferred_element_type=F32), 0.0)
        at = 0
        for f, r, count in pieces:
            piece = out[at : at + count * columns].reshape(count, columns, channels)
            at += count * columns
            if r < 0:
                piece = jnp.concatenate([piece[0:1] * above, piece[1:]], axis=0)
            if r + count > rows:
                piece = jnp.concatenate([piece[: count - 1], piece[count - 1 :] * below], axis=0)
            spread(wide_two, f, r + 1, piece)

    loads[2].wait()
    for f in range(2):
        for r, count in chunks(1, rows - 1):
            first([(f, r, count)])

    pl.semaphore_wait(barrier, devices - 1)

    @pl.when(s < strips - 1)
    def _():
        down.start()

    @pl.when(s > 0)
    def _():
        up.start()

    totals = [jnp.zeros((1, channels), F32) for f in range(2)]

    def second(pieces):
        lhs = [taps(wide_two, f, r, count) for f, r, count in pieces]
        lhs = lhs[0] if len(lhs) == 1 else jnp.concatenate(lhs, axis=0)
        out = jnp.dot(lhs, w_two[...], preferred_element_type=F32)
        at = 0
        for f, r, count in pieces:
            skip = maps[f, r : r + count].reshape(count * columns, channels).astype(F32)
            piece = jnp.maximum(skip + out[at : at + count * columns], 0.0)
            at += count * columns
            block_ref[f, 0, r : r + count] = piece.reshape(count, columns, channels)
            totals[f] = totals[f] + jnp.sum(piece, axis=0, keepdims=True)

    loads[3].wait()
    for f in range(2):
        for r, count in chunks(2, rows - 2):
            second([(f, r, count)])

    @pl.when(s < strips - 1)
    def _():
        down.wait_send()
        up.wait_recv()

    @pl.when(s > 0)
    def _():
        up.wait_send()
        down.wait_recv()

    for f in range(2):
        spread(wide_one, f, 0, jnp.maximum(halo[0, f].astype(F32), 0.0))
        spread(wide_one, f, rows + 2, jnp.maximum(halo[1, f].astype(F32), 0.0))
    edges = [(f, r) for f in range(2) for r in (0, rows)]
    first([(f, r - 1, 2) for f, r in edges])
    second([(f, min(r, rows - 2), 2) for f, r in edges])
    loads[6].wait()
    loads[7].wait()
    cells = rows * strips * columns
    lines = [total[:, LANES * p : LANES * (p + 1)] / cells for total in totals for p in range(packs)]
    lines.append(jnp.full((1, LANES), index[0].astype(F32)))
    lines.append(jnp.full((1, LANES), temp[0]))
    lines.append(jnp.zeros((part.shape[0] - len(lines), LANES), F32))
    share = jnp.concatenate(lines, axis=0)
    part[...] = share
    parts[me] = share

    def send(k, carry):
        other = lax.rem(me + k, devices)
        pltpu.make_async_remote_copy(
            src_ref=part, dst_ref=parts.at[me], send_sem=part_send, recv_sem=part_recv,
            device_id=(other // strips, lax.rem(other, strips)), device_id_type=MESH,
        ).start()
        return carry

    lax.fori_loop(1, devices, send, 0)
    loads[4].wait()
    loads[5].wait()
    others = parts.at[0 : devices - 1]
    everyone = pltpu.make_async_copy(others, others, part_recv)
    everyone.wait()
    gathered_ref[...] = parts[...]
    pltpu.make_async_copy(others, others, part_send).wait()


def unit_of(emb):
    inverse = lax.rsqrt(jnp.sum(emb * emb, axis=-1, keepdims=True) + 1e-06)
    return emb * inverse, inverse


def dot(left, right, over):
    return lax.dot_general(left, right, ((over[0:1], over[1:2]), ((), ())), preferred_element_type=F32)


def head_kernel(
    strips, block_ref, gathered_ref, sproj_ref, gproj_ref,
    loss_ref, sgrad_ref, ggrad_ref, out_ref,
    loss, sgrad, ggrad, sem,
):
    keep = pltpu.make_async_copy(block_ref, out_ref, sem.at[0])
    keep.start()
    batches = gathered_ref.shape[0] // strips
    packs = sproj_ref.shape[0] // LANES
    told = gathered_ref[...].reshape((batches, strips) + gathered_ref.shape[1:])
    heard = told[:, 0]
    for i in range(1, strips):
        heard = heard + told[:, i]
    heard = heard.astype(BF).astype(F32)

    def column(p):
        return jnp.concatenate([heard[i, p : p + 1] for i in range(batches)], axis=0)

    state_pool = jnp.concatenate([column(p) for p in range(packs)], axis=1).astype(BF)
    goal_pool = jnp.concatenate([column(packs + p) for p in range(packs)], axis=1).astype(BF)
    index = jnp.concatenate([told[i, 0, 2 * packs : 2 * packs + 1] for i in range(batches)], axis=0)[:, 0:1]
    sharpness = told[0, 0, 2 * packs + 1 : 2 * packs + 2, 0:1]
    state_unit, state_inverse = unit_of(dot(state_pool, sproj_ref[...], (1, 0)))
    goal_unit, goal_inverse = unit_of(dot(goal_pool, gproj_ref[...], (1, 0)))
    state_bf = state_unit.astype(BF)
    goal_bf = goal_unit.astype(BF)
    logits = sharpness * dot(state_bf, goal_bf, (1, 1))
    exp_logits = jnp.exp(logits)
    row_total = jnp.sum(exp_logits, axis=1, keepdims=True)
    matched = lax.broadcasted_iota(jnp.int32, logits.shape, 1).astype(F32) == index
    positive = jnp.sum(jnp.where(matched, logits, 0.0), axis=1, keepdims=True)
    losses = jnp.log(row_total) - positive
    mine = lax.broadcasted_iota(jnp.int32, losses.shape, 0) == lax.axis_index("batch")
    loss[0] = jnp.sum(jnp.where(mine, losses, 0.0))
    say = pltpu.make_async_copy(loss, loss_ref, sem.at[1])
    say.start()
    logit_grad = (exp_logits / row_total - matched.astype(F32)).astype(BF)
    copies = [keep, say]
    for pool, unit, inverse, unit_grad, grad, target in (
        (state_pool, state_unit, state_inverse, dot(logit_grad, goal_bf, (1, 0)), sgrad, sgrad_ref),
        (goal_pool, goal_unit, goal_inverse, dot(logit_grad, state_bf, (0, 0)), ggrad, ggrad_ref),
    ):
        unit_grad = sharpness * unit_grad
        along = jnp.sum(unit * unit_grad, axis=-1, keepdims=True)
        emb_grad = ((unit_grad - unit * along) * inverse).astype(BF)
        for p in range(packs):
            span = slice(LANES * p, LANES * (p + 1))
            grad[span] = dot(pool[:, span], emb_grad, (0, 0))
            copies.append(pltpu.make_async_copy(grad.at[span], target.at[span], sem.at[len(copies)]))
            copies[-1].start()
    for copy in copies:
        copy.wait()


def shards(batches, strips, state_maps, goal_maps, conv_one, conv_two, state_proj, goal_proj, inv_temp, pair_index):
    _, rows, columns, channels = state_maps.shape
    width = state_proj.shape[1]
    taps_in = conv_one.shape[0] * conv_one.shape[1] * channels
    any_spec = pl.BlockSpec(memory_space=pl.ANY)
    vmem = pl.BlockSpec(memory_space=pltpu.VMEM)
    block_shape = (2, 1, rows, columns, channels)
    dma = pltpu.SemaphoreType.DMA
    lines = 8 * pl.cdiv(2 * channels // LANES + 2, 8)
    stay = [
        pltpu.with_memory_space_constraint(value, pltpu.HBM)
        for value in (
            state_maps, goal_maps,
            conv_one.reshape(taps_in, channels), conv_two.reshape(taps_in, channels),
            state_proj, goal_proj,
        )
    ]
    held = pl.pallas_call(
        functools.partial(block_kernel, batches, strips),
        out_shape=(
            pltpu.VMEM(block_shape, F32),
            pltpu.VMEM((batches * strips, lines, LANES), F32),
            pltpu.VMEM((channels, width), BF),
            pltpu.VMEM((channels, width), BF),
        ),
        in_specs=[any_spec] * 8,
        out_specs=(vmem,) * 4,
        scratch_shapes=[
            pltpu.VMEM((2, rows, columns, channels), BF),
            pltpu.VMEM((2, rows + 4, columns, 3 * channels), BF),
            pltpu.VMEM((2, rows + 2, columns, 3 * channels), BF),
            pltpu.VMEM((taps_in, channels), BF),
            pltpu.VMEM((taps_in, channels), BF),
            pltpu.VMEM((2, 2, 2, columns, channels), BF),
            pltpu.SMEM((1,), jnp.int32),
            pltpu.SMEM((1,), F32),
            pltpu.VMEM((lines, LANES), F32),
            pltpu.VMEM((batches * strips, lines, LANES), F32),
            dma((8,)), dma((2,)), dma((2,)), dma(()), dma(()),
        ],
        compiler_params=pltpu.CompilerParams(
            collective_id=0, has_side_effects=True, vmem_limit_bytes=40 * 2**20
        ),
        name="block",
    )(*stay, pair_index, inv_temp)
    held = [pltpu.with_memory_space_constraint(value, pltpu.VMEM) for value in held]
    return pl.pallas_call(
        functools.partial(head_kernel, strips),
        out_shape=(
            jax.ShapeDtypeStruct((1,), F32),
            jax.ShapeDtypeStruct((channels, width), F32),
            jax.ShapeDtypeStruct((channels, width), F32),
            jax.ShapeDtypeStruct(block_shape, F32),
        ),
        in_specs=[vmem] * 4,
        out_specs=(any_spec,) * 4,
        scratch_shapes=[
            pltpu.SMEM((1,), F32),
            pltpu.VMEM((channels, width), F32),
            pltpu.VMEM((channels, width), F32),
            dma((2 + 2 * (channels // LANES),)),
        ],
        compiler_params=pltpu.CompilerParams(vmem_limit_bytes=40 * 2**20),
        name="head",
    )(*held)


def solution(mesh):
    placed = (
        P("batch", "strip", None, None),
        P("batch", "strip", None, None),
        P(),
        P(),
        P(),
        P(),
        P(),
        P("batch"),
    )
    return jax.shard_map(
        functools.partial(shards, mesh.shape["batch"], mesh.shape["strip"]),
        mesh=mesh,
        in_specs=placed,
        out_specs=(P("batch"), P(), P(), P(None, "batch", "strip", None, None)),
        check_vma=False,
    )
```

```python
import functools

import jax
import jax.numpy as jnp
from jax import lax
from jax.experimental import pallas as pl
from jax.experimental.pallas import tpu as pltpu
from jax.sharding import PartitionSpec as P

MESH = pl.DeviceIdType.MESH
BF = jnp.bfloat16
F32 = jnp.float32
LANES = 128
PAD = 8


def taps(store, k, frame, row, rows):
    pairs, channels = store.shape[3], store.shape[4]
    return jnp.concatenate(
        [store[k, frame, row + d : row + d + rows].reshape(rows * pairs, channels) for d in range(3)],
        axis=1,
    )


def stage(raw, frame, row, cells):
    columns = cells.shape[1]
    cells = cells.astype(F32)
    for h in range(raw.shape[2]):
        raw[frame, row : row + cells.shape[0], h, PAD : PAD + columns] = cells[:, :, LANES * h : LANES * (h + 1)]


def halved(raw, frame, row, first):
    pairs = (raw.shape[3] - 2 * PAD) // 2
    return [raw[frame, row, h, pl.ds(PAD + first, pairs, stride=2)] for h in range(raw.shape[2])]


def widen(store, raw, frame, rows):
    for row in rows:
        parts = [[jnp.maximum(x, 0.0) for x in halved(raw, frame, row, first)] for first in (-1, 0, 1, 2)]
        for h, (before, even, odd, after) in enumerate(zip(*parts)):
            lanes = slice(LANES * h, LANES * (h + 1))
            for k, value in enumerate((before - odd, even + odd, odd - even, even - after)):
                store[k, frame, row, :, lanes] = value.astype(BF)


def spread(store, frame, row, even, odd):
    rows, pairs, _ = even.shape
    where = lax.broadcasted_iota(jnp.int32, even.shape, 1)
    before = jnp.where(where == 0, 0.0, pltpu.roll(odd, 1, axis=1))
    after = jnp.where(where == pairs - 1, 0.0, pltpu.roll(even, pairs - 1, axis=1))
    span = slice(row, row + rows)
    for k, value in enumerate((before - odd, even + odd, odd - even, even - after)):
        store[k, frame, span] = value.astype(BF)


def mix(mixed, w):
    channels = w.shape[1]
    for d in range(3):
        left, centre, right = (
            w[(3 * d + c) * channels : (3 * d + c + 1) * channels].astype(F32) for c in range(3)
        )
        outer, inner = 0.5 * (left + right), 0.5 * centre
        span = slice(d * channels, (d + 1) * channels)
        mixed[0, span] = (outer + inner).astype(BF)
        mixed[1, span] = (outer - inner).astype(BF)


def products(store, w, mixed, pieces):
    channels = w.shape[1]
    out = []
    for k in range(4):
        lhs = [taps(store, k, f, r, count) for f, r, count in pieces]
        lhs = lhs[0] if len(lhs) == 1 else jnp.concatenate(lhs, axis=0)
        if k in (0, 3):
            c = 0 if k == 0 else 2
            rhs = jnp.concatenate(
                [w[(3 * d + c) * channels : (3 * d + c + 1) * channels] for d in range(3)], axis=0
            )
        else:
            rhs = mixed[k - 1]
        out.append(jnp.dot(lhs, rhs, preferred_element_type=F32))
    return (out[1] + out[2]) + out[0], (out[1] - out[2]) - out[3]


def block_kernel(
    batches, strips,
    state_ref, goal_ref, one_ref, two_ref, sproj_ref, gproj_ref, index_ref, temp_ref,
    block_ref, gathered_ref, sproj_out, gproj_out,
    maps, raw, wide_one, wide_two, w_one, w_two, mixed_one, mixed_two, halo, index, temp, part, parts,
    load_sem, halo_send, halo_recv, part_send, part_recv,
):
    b = lax.axis_index("batch")
    s = lax.axis_index("strip")
    rows, columns, channels = maps.shape[1], maps.shape[2], maps.shape[3]
    packs = channels // LANES
    devices = batches * strips
    me = b * strips + s

    loads = [
        pltpu.make_async_copy(source, target, load_sem.at[i])
        for i, (source, target) in enumerate((
            (state_ref.at[0], maps.at[0]),
            (one_ref, w_one),
            (goal_ref.at[0], maps.at[1]),
            (two_ref, w_two),
            (sproj_ref, sproj_out),
            (gproj_ref, gproj_out),
            (index_ref, index),
            (temp_ref, temp),
        ))
    ]
    for copy in loads:
        copy.start()

    @pl.when(s == 0)
    def _():
        halo[0] = jnp.zeros(halo.shape[1:], BF)

    @pl.when(s == strips - 1)
    def _():
        halo[1] = jnp.zeros(halo.shape[1:], BF)

    barrier = pltpu.get_barrier_semaphore()

    def greet(k, carry):
        other = lax.rem(me + k, devices)
        pl.semaphore_signal(
            barrier, inc=1, device_id=(other // strips, lax.rem(other, strips)), device_id_type=MESH
        )
        return carry

    lax.fori_loop(1, devices, greet, 0)
    edge = jnp.zeros((raw.shape[1], raw.shape[2], PAD, LANES), F32)
    for f in range(2):
        raw[f, :, :, 0:PAD] = edge
        raw[f, :, :, PAD + columns :] = edge

    loads[0].wait()
    stage(raw, 0, 2, maps[0])
    widen(wide_one, raw, 0, range(2, rows + 2))
    loads[1].wait()
    mix(mixed_one, w_one)
    loads[2].wait()
    stage(raw, 1, 2, maps[1])
    down = pltpu.make_async_remote_copy(
        src_ref=maps.at[:, rows - 2 : rows], dst_ref=halo.at[0],
        send_sem=halo_send.at[0], recv_sem=halo_recv.at[0],
        device_id=(b, lax.rem(s + 1, strips)), device_id_type=MESH,
    )
    up = pltpu.make_async_remote_copy(
        src_ref=maps.at[:, 0:2], dst_ref=halo.at[1],
        send_sem=halo_send.at[1], recv_sem=halo_recv.at[1],
        device_id=(b, lax.rem(s + strips - 1, strips)), device_id_type=MESH,
    )

    above = jnp.where(s > 0, 1.0, 0.0)
    below = jnp.where(s < strips - 1, 1.0, 0.0)

    pairs = columns // 2

    def first(pieces):
        evens, odds = products(wide_one, w_one, mixed_one, [(f, r + 1, count) for f, r, count in pieces])
        at = 0
        for f, r, count in pieces:
            both = []
            for out in (evens, odds):
                piece = jnp.maximum(out[at : at + count * pairs], 0.0).reshape(count, pairs, channels)
                if r < 0:
                    piece = jnp.concatenate([piece[0:1] * above, piece[1:]], axis=0)
                if r + count > rows:
                    piece = jnp.concatenate([piece[: count - 1], piece[count - 1 :] * below], axis=0)
                both.append(piece)
            at += count * pairs
            spread(wide_two, f, r + 1, *both)

    first([(0, 1, rows - 2)])
    widen(wide_one, raw, 1, range(2, rows + 2))
    first([(1, 1, rows - 2)])
    loads[3].wait()
    mix(mixed_two, w_two)

    def second(pieces):
        evens, odds = products(wide_two, w_two, mixed_two, pieces)
        at = 0
        for f, r, count in pieces:
            for first, out in enumerate((evens, odds)):
                piece = out[at : at + count * pairs]
                for i in range(count):
                    skips = halved(raw, f, r + 2 + i, first)
                    for h, skip in enumerate(skips):
                        lanes = slice(LANES * h, LANES * (h + 1))
                        value = jnp.maximum(skip + piece[i * pairs : (i + 1) * pairs, lanes], 0.0)
                        block_ref[f, r + i, h, pl.ds(first, pairs, stride=2)] = value
                        totals[f][h] = totals[f][h] + value
            at += count * pairs

    totals = [[jnp.zeros((pairs, LANES), F32) for h in range(packs)] for f in range(2)]
    second([(0, 2, rows - 4)])

    pl.semaphore_wait(barrier, devices - 1)

    @pl.when(s < strips - 1)
    def _():
        down.start()

    @pl.when(s > 0)
    def _():
        up.start()

    second([(1, 2, rows - 4)])

    @pl.when(s < strips - 1)
    def _():
        down.wait_send()
        up.wait_recv()

    @pl.when(s > 0)
    def _():
        up.wait_send()
        down.wait_recv()

    for f in range(2):
        stage(raw, f, 0, halo[0, f])
        stage(raw, f, rows + 2, halo[1, f])
        widen(wide_one, raw, f, (0, 1, rows + 2, rows + 3))
    edges = [(f, r) for f in range(2) for r in (0, rows)]
    first([(f, r - 1, 2) for f, r in edges])
    second([(f, min(r, rows - 2), 2) for f, r in edges])
    loads[6].wait()
    loads[7].wait()
    cells = rows * strips * columns
    lines = [jnp.sum(total, axis=0, keepdims=True) / cells for frame in totals for total in frame]
    lines.append(jnp.full((1, LANES), index[0].astype(F32)))
    lines.append(jnp.full((1, LANES), temp[0]))
    lines.append(jnp.zeros((part.shape[0] - len(lines), LANES), F32))
    share = jnp.concatenate(lines, axis=0)
    part[...] = share
    parts[me] = share

    facing = devices - 1 - me
    way = devices - 1 - (devices - 2) * (2 * me // devices)

    def send(k, carry):
        other = lax.rem(facing + k * way, devices)

        @pl.when(other != me)
        def _():
            pltpu.make_async_remote_copy(
                src_ref=part, dst_ref=parts.at[me], send_sem=part_send, recv_sem=part_recv,
                device_id=(other // strips, lax.rem(other, strips)), device_id_type=MESH,
            ).start()

        return carry

    lax.fori_loop(0, devices, send, 0)
    loads[4].wait()
    loads[5].wait()
    others = parts.at[0 : devices - 1]
    everyone = pltpu.make_async_copy(others, others, part_recv)
    everyone.wait()
    gathered_ref[...] = parts[...]
    pltpu.make_async_copy(others, others, part_send).wait()


def unit_of(emb):
    inverse = lax.rsqrt(jnp.sum(emb * emb, axis=-1, keepdims=True) + 1e-06)
    return emb * inverse, inverse


def dot(left, right, over):
    return lax.dot_general(left, right, ((over[0:1], over[1:2]), ((), ())), preferred_element_type=F32)


def head_kernel(
    strips, block_ref, gathered_ref, sproj_ref, gproj_ref,
    loss_ref, sgrad_ref, ggrad_ref, out_ref,
    loss, sgrad, ggrad, sem,
):
    copies = [
        pltpu.make_async_copy(
            block_ref.at[:, :, h], out_ref.at[:, 0, :, :, LANES * h : LANES * (h + 1)], sem.at[h]
        )
        for h in range(block_ref.shape[2])
    ]
    for copy in copies:
        copy.start()
    batches = gathered_ref.shape[0] // strips
    packs = sproj_ref.shape[0] // LANES
    told = gathered_ref[...].reshape((batches, strips) + gathered_ref.shape[1:])
    heard = told[:, 0]
    for i in range(1, strips):
        heard = heard + told[:, i]
    heard = heard.astype(BF).astype(F32)

    def column(p):
        return jnp.concatenate([heard[i, p : p + 1] for i in range(batches)], axis=0)

    state_pool = jnp.concatenate([column(p) for p in range(packs)], axis=1).astype(BF)
    goal_pool = jnp.concatenate([column(packs + p) for p in range(packs)], axis=1).astype(BF)
    index = jnp.concatenate([told[i, 0, 2 * packs : 2 * packs + 1] for i in range(batches)], axis=0)[:, 0:1]
    sharpness = told[0, 0, 2 * packs + 1 : 2 * packs + 2, 0:1]
    state_unit, state_inverse = unit_of(dot(state_pool, sproj_ref[...], (1, 0)))
    goal_unit, goal_inverse = unit_of(dot(goal_pool, gproj_ref[...], (1, 0)))
    state_bf = state_unit.astype(BF)
    goal_bf = goal_unit.astype(BF)
    logits = sharpness * dot(state_bf, goal_bf, (1, 1))
    exp_logits = jnp.exp(logits)
    row_total = jnp.sum(exp_logits, axis=1, keepdims=True)
    matched = lax.broadcasted_iota(jnp.int32, logits.shape, 1).astype(F32) == index
    positive = jnp.sum(jnp.where(matched, logits, 0.0), axis=1, keepdims=True)
    losses = jnp.log(row_total) - positive
    mine = lax.broadcasted_iota(jnp.int32, losses.shape, 0) == lax.axis_index("batch")
    loss[0] = jnp.sum(jnp.where(mine, losses, 0.0))
    copies.append(pltpu.make_async_copy(loss, loss_ref, sem.at[len(copies)]))
    copies[-1].start()
    logit_grad = (exp_logits / row_total - matched.astype(F32)).astype(BF)
    for pool, unit, inverse, unit_grad, grad, target in (
        (state_pool, state_unit, state_inverse, dot(logit_grad, goal_bf, (1, 0)), sgrad, sgrad_ref),
        (goal_pool, goal_unit, goal_inverse, dot(logit_grad, state_bf, (0, 0)), ggrad, ggrad_ref),
    ):
        unit_grad = sharpness * unit_grad
        along = jnp.sum(unit * unit_grad, axis=-1, keepdims=True)
        emb_grad = ((unit_grad - unit * along) * inverse).astype(BF)
        for p in range(packs):
            span = slice(LANES * p, LANES * (p + 1))
            grad[span] = dot(pool[:, span], emb_grad, (0, 0))
            copies.append(pltpu.make_async_copy(grad.at[span], target.at[span], sem.at[len(copies)]))
            copies[-1].start()
    for copy in copies:
        copy.wait()


def shards(batches, strips, state_maps, goal_maps, conv_one, conv_two, state_proj, goal_proj, inv_temp, pair_index):
    _, rows, columns, channels = state_maps.shape
    width = state_proj.shape[1]
    taps_in = conv_one.shape[0] * conv_one.shape[1] * channels
    any_spec = pl.BlockSpec(memory_space=pl.ANY)
    vmem = pl.BlockSpec(memory_space=pltpu.VMEM)
    packs = channels // LANES
    dma = pltpu.SemaphoreType.DMA
    lines = 8 * pl.cdiv(2 * channels // LANES + 2, 8)
    stay = [
        pltpu.with_memory_space_constraint(value, pltpu.HBM)
        for value in (
            state_maps, goal_maps,
            conv_one.reshape(taps_in, channels), conv_two.reshape(taps_in, channels),
            state_proj, goal_proj,
        )
    ]
    held = pl.pallas_call(
        functools.partial(block_kernel, batches, strips),
        out_shape=(
            pltpu.VMEM((2, rows, packs, columns, LANES), F32),
            pltpu.VMEM((batches * strips, lines, LANES), F32),
            pltpu.VMEM((channels, width), BF),
            pltpu.VMEM((channels, width), BF),
        ),
        in_specs=[any_spec] * 8,
        out_specs=(vmem,) * 4,
        scratch_shapes=[
            pltpu.VMEM((2, rows, columns, channels), BF),
            pltpu.VMEM((2, rows + 4, packs, columns + 2 * PAD, LANES), F32),
            pltpu.VMEM((4, 2, rows + 4, columns // 2, channels), BF),
            pltpu.VMEM((4, 2, rows + 2, columns // 2, channels), BF),
            pltpu.VMEM((taps_in, channels), BF),
            pltpu.VMEM((taps_in, channels), BF),
            pltpu.VMEM((2, taps_in // 3, channels), BF),
            pltpu.VMEM((2, taps_in // 3, channels), BF),
            pltpu.VMEM((2, 2, 2, columns, channels), BF),
            pltpu.SMEM((1,), jnp.int32),
            pltpu.SMEM((1,), F32),
            pltpu.VMEM((lines, LANES), F32),
            pltpu.VMEM((batches * strips, lines, LANES), F32),
            dma((8,)), dma((2,)), dma((2,)), dma(()), dma(()),
        ],
        compiler_params=pltpu.CompilerParams(
            collective_id=0, has_side_effects=True, vmem_limit_bytes=40 * 2**20
        ),
        name="block",
    )(*stay, pair_index, inv_temp)
    held = [pltpu.with_memory_space_constraint(value, pltpu.VMEM) for value in held]
    return pl.pallas_call(
        functools.partial(head_kernel, strips),
        out_shape=(
            jax.ShapeDtypeStruct((1,), F32),
            jax.ShapeDtypeStruct((channels, width), F32),
            jax.ShapeDtypeStruct((channels, width), F32),
            jax.ShapeDtypeStruct((2, 1, rows, columns, channels), F32),
        ),
        in_specs=[vmem] * 4,
        out_specs=(any_spec,) * 4,
        scratch_shapes=[
            pltpu.SMEM((1,), F32),
            pltpu.VMEM((channels, width), F32),
            pltpu.VMEM((channels, width), F32),
            dma((1 + 3 * (channels // LANES),)),
        ],
        compiler_params=pltpu.CompilerParams(vmem_limit_bytes=40 * 2**20),
        name="head",
    )(*held)


def solution(mesh):
    placed = (
        P("batch", "strip", None, None),
        P("batch", "strip", None, None),
        P(),
        P(),
        P(),
        P(),
        P(),
        P("batch"),
    )
    return jax.shard_map(
        functools.partial(shards, mesh.shape["batch"], mesh.shape["strip"]),
        mesh=mesh,
        in_specs=placed,
        out_specs=(P("batch"), P(), P(), P(None, "batch", "strip", None, None)),
        check_vma=False,
    )
```

```python
import functools

import jax
import jax.numpy as jnp
from jax import lax
from jax.experimental import pallas as pl
from jax.experimental.pallas import tpu as pltpu
from jax.sharding import PartitionSpec as P

MESH = pl.DeviceIdType.MESH
BF = jnp.bfloat16
F32 = jnp.float32
LANES = 128
PAD = 8


def taps(store, k, frame, row, rows):
    pairs, channels = store.shape[3], store.shape[4]
    return jnp.concatenate(
        [store[k, frame, row + d : row + d + rows].reshape(rows * pairs, channels) for d in range(3)],
        axis=1,
    )


def stage(raw, frame, row, cells):
    columns = cells.shape[1]
    cells = cells.astype(F32)
    for h in range(raw.shape[2]):
        raw[frame, row : row + cells.shape[0], h, PAD : PAD + columns] = cells[:, :, LANES * h : LANES * (h + 1)]


def halved(raw, frame, row, first):
    pairs = (raw.shape[3] - 2 * PAD) // 2
    return [raw[frame, row, h, pl.ds(PAD + first, pairs, stride=2)] for h in range(raw.shape[2])]


def widen(store, raw, frame, rows):
    for row in rows:
        parts = [[jnp.maximum(x, 0.0) for x in halved(raw, frame, row, first)] for first in (-1, 0, 1, 2)]
        for h, (before, even, odd, after) in enumerate(zip(*parts)):
            lanes = slice(LANES * h, LANES * (h + 1))
            for k, value in enumerate((before - odd, even + odd, odd - even, even - after)):
                store[k, frame, row, :, lanes] = value.astype(BF)


def spread(store, frame, row, even, odd):
    rows, pairs, _ = even.shape
    where = lax.broadcasted_iota(jnp.int32, even.shape, 1)
    before = jnp.where(where == 0, 0.0, pltpu.roll(odd, 1, axis=1))
    after = jnp.where(where == pairs - 1, 0.0, pltpu.roll(even, pairs - 1, axis=1))
    span = slice(row, row + rows)
    for k, value in enumerate((before - odd, even + odd, odd - even, even - after)):
        store[k, frame, span] = value.astype(BF)


def mix(mixed, w):
    channels = w.shape[1]
    for d in range(3):
        left, centre, right = (
            w[(3 * d + c) * channels : (3 * d + c + 1) * channels].astype(F32) for c in range(3)
        )
        outer, inner = 0.5 * (left + right), 0.5 * centre
        span = slice(d * channels, (d + 1) * channels)
        mixed[0, span] = (outer + inner).astype(BF)
        mixed[1, span] = (outer - inner).astype(BF)


def products(store, w, mixed, pieces):
    channels = w.shape[1]
    out = []
    for k in range(4):
        lhs = [taps(store, k, f, r, count) for f, r, count in pieces]
        lhs = lhs[0] if len(lhs) == 1 else jnp.concatenate(lhs, axis=0)
        if k in (0, 3):
            c = 0 if k == 0 else 2
            rhs = jnp.concatenate(
                [w[(3 * d + c) * channels : (3 * d + c + 1) * channels] for d in range(3)], axis=0
            )
        else:
            rhs = mixed[k - 1]
        out.append(jnp.dot(lhs, rhs, preferred_element_type=F32))
    return (out[1] + out[2]) + out[0], (out[1] - out[2]) - out[3]


def block_kernel(
    batches, strips,
    state_ref, goal_ref, one_ref, two_ref, sproj_ref, gproj_ref, index_ref, temp_ref,
    block_ref, gathered_ref, marks_out, sproj_out, gproj_out,
    maps, raw, wide_one, wide_two, w_one, w_two, mixed_one, mixed_two, halo, index, temp, mark, marks, part, parts,
    load_sem, halo_send, halo_recv, mark_send, mark_recv, part_send, part_recv,
):
    b = lax.axis_index("batch")
    s = lax.axis_index("strip")
    rows, columns, channels = maps.shape[1], maps.shape[2], maps.shape[3]
    packs = channels // LANES
    devices = batches * strips
    me = b * strips + s

    loads = [
        pltpu.make_async_copy(source, target, load_sem.at[i])
        for i, (source, target) in enumerate((
            (state_ref.at[0], maps.at[0]),
            (one_ref, w_one),
            (goal_ref.at[0], maps.at[1]),
            (two_ref, w_two),
            (sproj_ref, sproj_out),
            (gproj_ref, gproj_out),
            (index_ref, index),
            (temp_ref, temp),
        ))
    ]
    for copy in loads:
        copy.start()

    @pl.when(s == 0)
    def _():
        halo[0] = jnp.zeros(halo.shape[1:], BF)

    @pl.when(s == strips - 1)
    def _():
        halo[1] = jnp.zeros(halo.shape[1:], BF)

    barrier = pltpu.get_barrier_semaphore()

    def greet(k, carry):
        other = lax.rem(me + k, devices)
        pl.semaphore_signal(
            barrier, inc=1, device_id=(other // strips, lax.rem(other, strips)), device_id_type=MESH
        )
        return carry

    lax.fori_loop(1, devices, greet, 0)
    edge = jnp.zeros((raw.shape[1], raw.shape[2], PAD, LANES), F32)
    for f in range(2):
        raw[f, :, :, 0:PAD] = edge
        raw[f, :, :, PAD + columns :] = edge

    loads[0].wait()
    stage(raw, 0, 2, maps[0])
    widen(wide_one, raw, 0, range(2, rows + 2))
    loads[1].wait()
    mix(mixed_one, w_one)
    loads[2].wait()
    stage(raw, 1, 2, maps[1])
    down = pltpu.make_async_remote_copy(
        src_ref=maps.at[:, rows - 2 : rows], dst_ref=halo.at[0],
        send_sem=halo_send.at[0], recv_sem=halo_recv.at[0],
        device_id=(b, lax.rem(s + 1, strips)), device_id_type=MESH,
    )
    up = pltpu.make_async_remote_copy(
        src_ref=maps.at[:, 0:2], dst_ref=halo.at[1],
        send_sem=halo_send.at[1], recv_sem=halo_recv.at[1],
        device_id=(b, lax.rem(s + strips - 1, strips)), device_id_type=MESH,
    )

    above = jnp.where(s > 0, 1.0, 0.0)
    below = jnp.where(s < strips - 1, 1.0, 0.0)

    pairs = columns // 2

    def first(pieces):
        evens, odds = products(wide_one, w_one, mixed_one, [(f, r + 1, count) for f, r, count in pieces])
        at = 0
        for f, r, count in pieces:
            both = []
            for out in (evens, odds):
                piece = jnp.maximum(out[at : at + count * pairs], 0.0).reshape(count, pairs, channels)
                if r < 0:
                    piece = jnp.concatenate([piece[0:1] * above, piece[1:]], axis=0)
                if r + count > rows:
                    piece = jnp.concatenate([piece[: count - 1], piece[count - 1 :] * below], axis=0)
                both.append(piece)
            at += count * pairs
            spread(wide_two, f, r + 1, *both)

    def second(pieces):
        evens, odds = products(wide_two, w_two, mixed_two, pieces)
        at = 0
        for f, r, count in pieces:
            for first, out in enumerate((evens, odds)):
                piece = out[at : at + count * pairs]
                for i in range(count):
                    skips = halved(raw, f, r + 2 + i, first)
                    for h, skip in enumerate(skips):
                        lanes = slice(LANES * h, LANES * (h + 1))
                        value = jnp.maximum(skip + piece[i * pairs : (i + 1) * pairs, lanes], 0.0)
                        block_ref[f, r + i, h, pl.ds(first, pairs, stride=2)] = value
                        totals[f][h] = totals[f][h] + value
            at += count * pairs

    totals = [[jnp.zeros((pairs, LANES), F32) for h in range(packs)] for f in range(2)]
    first([(0, 1, rows - 2)])
    widen(wide_one, raw, 1, range(2, rows + 2))
    first([(1, 1, rows - 2)])

    pl.semaphore_wait(barrier, devices - 1)
    loads[6].wait()
    told = jnp.full(mark.shape, index[0].astype(F32))
    mark[...] = told
    marks[b] = told
    own = 2 * b // batches
    way = batches - 1 - (batches - 2) * own
    first_peer = (batches - 1) * (1 - own)

    def peers(make):
        def one(k, carry):
            other = lax.rem(first_peer + k * way, batches)

            @pl.when(other != b)
            def _():
                make(other).start()

            return carry

        lax.fori_loop(0, batches, one, 0)

    def settle(buffer, sem, count):
        if count:
            pltpu.make_async_copy(buffer.at[0:count], buffer.at[0:count], sem).wait()

    peers(lambda other: pltpu.make_async_remote_copy(
        src_ref=mark, dst_ref=marks.at[b], send_sem=mark_send, recv_sem=mark_recv,
        device_id=(other, s), device_id_type=MESH,
    ))

    @pl.when(s < strips - 1)
    def _():
        down.start()

    @pl.when(s > 0)
    def _():
        up.start()

    loads[3].wait()
    mix(mixed_two, w_two)
    second([(0, 2, rows - 4)])
    second([(1, 2, rows - 4)])

    @pl.when(s < strips - 1)
    def _():
        down.wait_send()
        up.wait_recv()

    @pl.when(s > 0)
    def _():
        up.wait_send()
        down.wait_recv()

    for f in range(2):
        stage(raw, f, 0, halo[0, f])
        stage(raw, f, rows + 2, halo[1, f])
        widen(wide_one, raw, f, (0, 1, rows + 2, rows + 3))
    edges = [(f, r) for f in range(2) for r in (0, rows)]
    first([(f, r - 1, 2) for f, r in edges])
    second([(f, min(r, rows - 2), 2) for f, r in edges])
    cells = rows * strips * columns
    lines = [jnp.sum(total, axis=0, keepdims=True) / cells for frame in totals for total in frame]
    share = jnp.concatenate(lines, axis=0)
    part[...] = share
    parts[me] = share
    high = 2 * me // devices
    stride = devices - 1 - (devices - 2) * high
    nearest = (devices - 1) * (1 - high)

    def send(k, carry):
        other = lax.rem(nearest + k * stride, devices)

        @pl.when(other != me)
        def _():
            pltpu.make_async_remote_copy(
                src_ref=part, dst_ref=parts.at[me], send_sem=part_send, recv_sem=part_recv,
                device_id=(other // strips, lax.rem(other, strips)), device_id_type=MESH,
            ).start()

        return carry

    lax.fori_loop(0, devices, send, 0)
    for i in (4, 5, 7):
        loads[i].wait()
    settle(marks, mark_recv, batches - 1)
    settle(marks, mark_send, batches - 1)
    marks_out[0:batches] = marks[...]
    marks_out[batches] = jnp.full(mark.shape, temp[0])
    settle(parts, part_recv, devices - 1)
    gathered_ref[...] = parts[...]
    settle(parts, part_send, devices - 1)


def unit_of(emb):
    inverse = lax.rsqrt(jnp.sum(emb * emb, axis=-1, keepdims=True) + 1e-06)
    return emb * inverse, inverse


def dot(left, right, over):
    return lax.dot_general(left, right, ((over[0:1], over[1:2]), ((), ())), preferred_element_type=F32)


def head_kernel(
    strips, block_ref, gathered_ref, marks_ref, sproj_ref, gproj_ref,
    loss_ref, sgrad_ref, ggrad_ref, out_ref,
    loss, sgrad, ggrad, sem,
):
    copies = [
        pltpu.make_async_copy(
            block_ref.at[:, :, h], out_ref.at[:, 0, :, :, LANES * h : LANES * (h + 1)], sem.at[h]
        )
        for h in range(block_ref.shape[2])
    ]
    for copy in copies:
        copy.start()
    batches = gathered_ref.shape[0] // strips
    packs = sproj_ref.shape[0] // LANES
    told = gathered_ref[...].reshape((batches, strips) + gathered_ref.shape[1:])
    heard = told[:, 0]
    for i in range(1, strips):
        heard = heard + told[:, i]
    heard = heard.astype(BF).astype(F32)

    def column(p):
        return jnp.concatenate([heard[i, p : p + 1] for i in range(batches)], axis=0)

    state_pool = jnp.concatenate([column(p) for p in range(packs)], axis=1).astype(BF)
    goal_pool = jnp.concatenate([column(packs + p) for p in range(packs)], axis=1).astype(BF)
    index = jnp.concatenate([marks_ref[i] for i in range(batches)], axis=0)[:, 0:1]
    sharpness = marks_ref[batches][:, 0:1]
    state_unit, state_inverse = unit_of(dot(state_pool, sproj_ref[...], (1, 0)))
    goal_unit, goal_inverse = unit_of(dot(goal_pool, gproj_ref[...], (1, 0)))
    state_bf = state_unit.astype(BF)
    goal_bf = goal_unit.astype(BF)
    logits = sharpness * dot(state_bf, goal_bf, (1, 1))
    exp_logits = jnp.exp(logits)
    row_total = jnp.sum(exp_logits, axis=1, keepdims=True)
    matched = lax.broadcasted_iota(jnp.int32, logits.shape, 1).astype(F32) == index
    positive = jnp.sum(jnp.where(matched, logits, 0.0), axis=1, keepdims=True)
    losses = jnp.log(row_total) - positive
    mine = lax.broadcasted_iota(jnp.int32, losses.shape, 0) == lax.axis_index("batch")
    loss[0] = jnp.sum(jnp.where(mine, losses, 0.0))
    copies.append(pltpu.make_async_copy(loss, loss_ref, sem.at[len(copies)]))
    copies[-1].start()
    logit_grad = (exp_logits / row_total - matched.astype(F32)).astype(BF)
    for pool, unit, inverse, unit_grad, grad, target in (
        (state_pool, state_unit, state_inverse, dot(logit_grad, goal_bf, (1, 0)), sgrad, sgrad_ref),
        (goal_pool, goal_unit, goal_inverse, dot(logit_grad, state_bf, (0, 0)), ggrad, ggrad_ref),
    ):
        unit_grad = sharpness * unit_grad
        along = jnp.sum(unit * unit_grad, axis=-1, keepdims=True)
        emb_grad = ((unit_grad - unit * along) * inverse).astype(BF)
        for p in range(packs):
            span = slice(LANES * p, LANES * (p + 1))
            grad[span] = dot(pool[:, span], emb_grad, (0, 0))
            copies.append(pltpu.make_async_copy(grad.at[span], target.at[span], sem.at[len(copies)]))
            copies[-1].start()
    for copy in copies:
        copy.wait()


def shards(batches, strips, state_maps, goal_maps, conv_one, conv_two, state_proj, goal_proj, inv_temp, pair_index):
    _, rows, columns, channels = state_maps.shape
    width = state_proj.shape[1]
    taps_in = conv_one.shape[0] * conv_one.shape[1] * channels
    any_spec = pl.BlockSpec(memory_space=pl.ANY)
    vmem = pl.BlockSpec(memory_space=pltpu.VMEM)
    packs = channels // LANES
    dma = pltpu.SemaphoreType.DMA
    lines = 2 * packs
    stay = [
        pltpu.with_memory_space_constraint(value, pltpu.HBM)
        for value in (
            state_maps, goal_maps,
            conv_one.reshape(taps_in, channels), conv_two.reshape(taps_in, channels),
            state_proj, goal_proj,
        )
    ]
    held = pl.pallas_call(
        functools.partial(block_kernel, batches, strips),
        out_shape=(
            pltpu.VMEM((2, rows, packs, columns, LANES), F32),
            pltpu.VMEM((batches * strips, lines, LANES), F32),
            pltpu.VMEM((batches + 1, 1, LANES), F32),
            pltpu.VMEM((channels, width), BF),
            pltpu.VMEM((channels, width), BF),
        ),
        in_specs=[any_spec] * 8,
        out_specs=(vmem,) * 5,
        scratch_shapes=[
            pltpu.VMEM((2, rows, columns, channels), BF),
            pltpu.VMEM((2, rows + 4, packs, columns + 2 * PAD, LANES), F32),
            pltpu.VMEM((4, 2, rows + 4, columns // 2, channels), BF),
            pltpu.VMEM((4, 2, rows + 2, columns // 2, channels), BF),
            pltpu.VMEM((taps_in, channels), BF),
            pltpu.VMEM((taps_in, channels), BF),
            pltpu.VMEM((2, taps_in // 3, channels), BF),
            pltpu.VMEM((2, taps_in // 3, channels), BF),
            pltpu.VMEM((2, 2, 2, columns, channels), BF),
            pltpu.SMEM((1,), jnp.int32),
            pltpu.SMEM((1,), F32),
            pltpu.VMEM((1, LANES), F32),
            pltpu.VMEM((batches, 1, LANES), F32),
            pltpu.VMEM((lines, LANES), F32),
            pltpu.VMEM((batches * strips, lines, LANES), F32),
            dma((8,)), dma((2,)), dma((2,)), dma(()), dma(()), dma(()), dma(()),
        ],
        compiler_params=pltpu.CompilerParams(
            collective_id=0, has_side_effects=True, vmem_limit_bytes=40 * 2**20
        ),
        name="block",
    )(*stay, pair_index, inv_temp)
    held = [pltpu.with_memory_space_constraint(value, pltpu.VMEM) for value in held]
    return pl.pallas_call(
        functools.partial(head_kernel, strips),
        out_shape=(
            jax.ShapeDtypeStruct((1,), F32),
            jax.ShapeDtypeStruct((channels, width), F32),
            jax.ShapeDtypeStruct((channels, width), F32),
            jax.ShapeDtypeStruct((2, 1, rows, columns, channels), F32),
        ),
        in_specs=[vmem] * 5,
        out_specs=(any_spec,) * 4,
        scratch_shapes=[
            pltpu.SMEM((1,), F32),
            pltpu.VMEM((channels, width), F32),
            pltpu.VMEM((channels, width), F32),
            dma((1 + 3 * (channels // LANES),)),
        ],
        compiler_params=pltpu.CompilerParams(vmem_limit_bytes=40 * 2**20),
        name="head",
    )(*held)


def solution(mesh):
    placed = (
        P("batch", "strip", None, None),
        P("batch", "strip", None, None),
        P(),
        P(),
        P(),
        P(),
        P(),
        P("batch"),
    )
    return jax.shard_map(
        functools.partial(shards, mesh.shape["batch"], mesh.shape["strip"]),
        mesh=mesh,
        in_specs=placed,
        out_specs=(P("batch"), P(), P(), P(None, "batch", "strip", None, None)),
        check_vma=False,
    )
```

```python
import functools

import jax
import jax.numpy as jnp
from jax import lax
from jax.experimental import pallas as pl
from jax.experimental.pallas import tpu as pltpu
from jax.sharding import PartitionSpec as P

MESH = pl.DeviceIdType.MESH
BF = jnp.bfloat16
F32 = jnp.float32
LANES = 128
PAD = 8


def taps(store, k, frame, row, rows):
    pairs, channels = store.shape[3], store.shape[4]
    return jnp.concatenate(
        [store[k, frame, row + d : row + d + rows].reshape(rows * pairs, channels) for d in range(3)],
        axis=1,
    )


def stage(raw, frame, row, cells):
    columns = cells.shape[1]
    cells = cells.astype(F32)
    for h in range(raw.shape[2]):
        raw[frame, row : row + cells.shape[0], h, PAD : PAD + columns] = cells[:, :, LANES * h : LANES * (h + 1)]


def halved(raw, frame, row, first):
    pairs = (raw.shape[3] - 2 * PAD) // 2
    return [raw[frame, row, h, pl.ds(PAD + first, pairs, stride=2)] for h in range(raw.shape[2])]


def widen(store, raw, frame, rows):
    for row in rows:
        parts = [[jnp.maximum(x, 0.0) for x in halved(raw, frame, row, first)] for first in (-1, 0, 1, 2)]
        for h, (before, even, odd, after) in enumerate(zip(*parts)):
            lanes = slice(LANES * h, LANES * (h + 1))
            for k, value in enumerate((before - odd, even + odd, odd - even, even - after)):
                store[k, frame, row, :, lanes] = value.astype(BF)


def spread(store, frame, row, even, odd):
    rows, pairs, _ = even.shape
    where = lax.broadcasted_iota(jnp.int32, even.shape, 1)
    before = jnp.where(where == 0, 0.0, pltpu.roll(odd, 1, axis=1))
    after = jnp.where(where == pairs - 1, 0.0, pltpu.roll(even, pairs - 1, axis=1))
    span = slice(row, row + rows)
    for k, value in enumerate((before - odd, even + odd, odd - even, even - after)):
        store[k, frame, span] = value.astype(BF)


def mix(mixed, w):
    channels = w.shape[1]
    for d in range(3):
        left, centre, right = (
            w[(3 * d + c) * channels : (3 * d + c + 1) * channels].astype(F32) for c in range(3)
        )
        outer, inner = 0.5 * (left + right), 0.5 * centre
        span = slice(d * channels, (d + 1) * channels)
        mixed[0, span] = (outer + inner).astype(BF)
        mixed[1, span] = (outer - inner).astype(BF)


def products(store, w, mixed, pieces):
    channels = w.shape[1]
    out = [None] * 4
    for k in (0, 3, 1, 2):
        lhs = [taps(store, k, f, r, count) for f, r, count in pieces]
        lhs = lhs[0] if len(lhs) == 1 else jnp.concatenate(lhs, axis=0)
        if k in (0, 3):
            c = 0 if k == 0 else 2
            rhs = jnp.concatenate(
                [w[(3 * d + c) * channels : (3 * d + c + 1) * channels] for d in range(3)], axis=0
            )
        else:
            rhs = mixed[k - 1]
        out[k] = jnp.dot(lhs, rhs, preferred_element_type=F32)
    return out


def combine(out):
    return (out[1] + out[2]) + out[0], (out[1] - out[2]) - out[3]


def block_kernel(
    batches, strips,
    state_ref, goal_ref, one_ref, two_ref, sproj_ref, gproj_ref, index_ref, temp_ref,
    block_ref, gathered_ref, marks_out, sproj_out, gproj_out,
    maps, raw, wide_one, wide_two, w_one, w_two, mixed_one, mixed_two, halo, index, temp, mark, marks, part, parts,
    load_sem, halo_send, halo_recv, mark_send, mark_recv, part_send, part_recv,
):
    b = lax.axis_index("batch")
    s = lax.axis_index("strip")
    rows, columns, channels = maps.shape[1], maps.shape[2], maps.shape[3]
    packs = channels // LANES
    devices = batches * strips
    me = b * strips + s

    loads = [
        pltpu.make_async_copy(source, target, load_sem.at[i])
        for i, (source, target) in enumerate((
            (state_ref.at[0], maps.at[0]),
            (goal_ref.at[0], maps.at[1]),
            (one_ref, w_one),
            (two_ref, w_two),
            (sproj_ref, sproj_out),
            (gproj_ref, gproj_out),
            (index_ref, index),
            (temp_ref, temp),
        ))
    ]
    for copy in loads:
        copy.start()

    @pl.when(s == 0)
    def _():
        halo[0] = jnp.zeros(halo.shape[1:], BF)

    @pl.when(s == strips - 1)
    def _():
        halo[1] = jnp.zeros(halo.shape[1:], BF)

    barrier = pltpu.get_barrier_semaphore()

    def greet(k, carry):
        other = lax.rem(b + k, batches)
        for t in range(strips):
            pl.semaphore_signal(barrier, inc=1, device_id=(other, t), device_id_type=MESH)
        return carry

    for t in range(1, strips):
        pl.semaphore_signal(barrier, inc=1, device_id=(b, lax.rem(s + t, strips)), device_id_type=MESH)
    lax.fori_loop(1, batches, greet, 0)
    edge = jnp.zeros((raw.shape[1], raw.shape[2], PAD, LANES), F32)
    for f in range(2):
        raw[f, :, :, 0:PAD] = edge
        raw[f, :, :, PAD + columns :] = edge

    down = pltpu.make_async_remote_copy(
        src_ref=maps.at[:, rows - 2 : rows], dst_ref=halo.at[0],
        send_sem=halo_send.at[0], recv_sem=halo_recv.at[0],
        device_id=(b, lax.rem(s + 1, strips)), device_id_type=MESH,
    )
    up = pltpu.make_async_remote_copy(
        src_ref=maps.at[:, 0:2], dst_ref=halo.at[1],
        send_sem=halo_send.at[1], recv_sem=halo_recv.at[1],
        device_id=(b, lax.rem(s + strips - 1, strips)), device_id_type=MESH,
    )

    above = jnp.where(s > 0, 1.0, 0.0)
    below = jnp.where(s < strips - 1, 1.0, 0.0)
    pairs = columns // 2
    inner = range(2, rows + 2)
    outer = (0, 1, rows + 2, rows + 3)
    totals = [[jnp.zeros((pairs, LANES), F32) for h in range(packs)] for f in range(2)]

    def first(pieces):
        return products(wide_one, w_one, mixed_one, [(f, r + 1, count) for f, r, count in pieces])

    def after_first(pieces, out):
        evens, odds = combine(out)
        at = 0
        for f, r, count in pieces:
            both = []
            for out in (evens, odds):
                piece = jnp.maximum(out[at : at + count * pairs], 0.0).reshape(count, pairs, channels)
                if r < 0:
                    piece = jnp.concatenate([piece[0:1] * above, piece[1:]], axis=0)
                if r + count > rows:
                    piece = jnp.concatenate([piece[: count - 1], piece[count - 1 :] * below], axis=0)
                both.append(piece)
            at += count * pairs
            spread(wide_two, f, r + 1, *both)

    def second(pieces):
        return products(wide_two, w_two, mixed_two, pieces)

    def after_second(pieces, out):
        evens, odds = combine(out)
        at = 0
        for f, r, count in pieces:
            for first, out in enumerate((evens, odds)):
                piece = out[at : at + count * pairs]
                for i in range(count):
                    skips = halved(raw, f, r + 2 + i, first)
                    for h, skip in enumerate(skips):
                        lanes = slice(LANES * h, LANES * (h + 1))
                        value = jnp.maximum(skip + piece[i * pairs : (i + 1) * pairs, lanes], 0.0)
                        block_ref[f, r + i, h, pl.ds(first, pairs, stride=2)] = value
                        totals[f][h] = totals[f][h] + value
            at += count * pairs

    loads[0].wait()
    stage(raw, 0, 2, maps[0])
    loads[1].wait()
    pl.semaphore_wait(barrier, devices - 1)

    @pl.when(s < strips - 1)
    def _():
        down.start()

    @pl.when(s > 0)
    def _():
        up.start()

    widen(wide_one, raw, 0, inner)
    loads[2].wait()
    mix(mixed_one, w_one)
    work = [
        [(0, 1, rows - 2)],
        [(0, -1, 2), (0, rows - 1, 2), (1, -1, rows // 2)],
        [(1, rows // 2 - 1, rows + 2 - rows // 2)],
    ]
    done_0 = first(work[0])
    stage(raw, 1, 2, maps[1])
    widen(wide_one, raw, 1, inner)
    loads[6].wait()
    told = jnp.full(mark.shape, index[0].astype(F32))
    mark[...] = told
    marks[b] = told
    own = 2 * b // batches
    way = batches - 1 - (batches - 2) * own
    first_peer = (batches - 1) * (1 - own)

    def peers(make):
        def one(k, carry):
            other = lax.rem(first_peer + k * way, batches)

            @pl.when(other != b)
            def _():
                make(other).start()

            return carry

        lax.fori_loop(0, batches, one, 0)

    def settle(buffer, sem, count):
        if count:
            pltpu.make_async_copy(buffer.at[0:count], buffer.at[0:count], sem).wait()

    peers(lambda other: pltpu.make_async_remote_copy(
        src_ref=mark, dst_ref=marks.at[b], send_sem=mark_send, recv_sem=mark_recv,
        device_id=(other, s), device_id_type=MESH,
    ))

    @pl.when(s < strips - 1)
    def _():
        down.wait_send()
        up.wait_recv()

    @pl.when(s > 0)
    def _():
        up.wait_send()
        down.wait_recv()

    loads[3].wait()
    for f in range(2):
        stage(raw, f, 0, halo[0, f])
        stage(raw, f, rows + 2, halo[1, f])
        widen(wide_one, raw, f, outer)
    done_1 = first(work[1])
    after_first(work[0], done_0)
    mix(mixed_two, w_two)
    done_2 = first(work[2])
    after_first(work[1], done_1)
    frames = [[(f, 0, rows)] for f in range(2)]
    out_0 = second(frames[0])
    after_first(work[2], done_2)
    out_1 = second(frames[1])
    after_second(frames[0], out_0)
    after_second(frames[1], out_1)
    cells = rows * strips * columns
    lines = [jnp.sum(total, axis=0, keepdims=True) / cells for frame in totals for total in frame]
    share = jnp.concatenate(lines, axis=0)
    part[...] = share
    parts[me] = share

    def send(other, t):
        pltpu.make_async_remote_copy(
            src_ref=part, dst_ref=parts.at[me], send_sem=part_send, recv_sem=part_recv,
            device_id=(other, t), device_id_type=MESH,
        ).start()

    def spray(k, carry):
        other = lax.rem(first_peer + k * way, batches)

        @pl.when(other != b)
        def _():
            for t in range(strips):
                send(other, t)

        return carry

    lax.fori_loop(0, batches, spray, 0)
    for t in range(1, strips):
        send(b, lax.rem(s + t, strips))
    for i in (4, 5, 7):
        loads[i].wait()
    settle(marks, mark_recv, batches - 1)
    settle(marks, mark_send, batches - 1)
    marks_out[0:batches] = marks[...]
    marks_out[batches] = jnp.full(mark.shape, temp[0])
    settle(parts, part_recv, devices - 1)
    gathered_ref[...] = parts[...]
    settle(parts, part_send, devices - 1)


def unit_of(emb):
    inverse = lax.rsqrt(jnp.sum(emb * emb, axis=-1, keepdims=True) + 1e-06)
    return emb * inverse, inverse


def dot(left, right, over):
    return lax.dot_general(left, right, ((over[0:1], over[1:2]), ((), ())), preferred_element_type=F32)


def head_kernel(
    strips, block_ref, gathered_ref, marks_ref, sproj_ref, gproj_ref,
    loss_ref, sgrad_ref, ggrad_ref, out_ref,
    loss, sgrad, ggrad, sem,
):
    copies = [
        pltpu.make_async_copy(
            block_ref.at[:, :, h], out_ref.at[:, 0, :, :, LANES * h : LANES * (h + 1)], sem.at[h]
        )
        for h in range(block_ref.shape[2])
    ]
    for copy in copies:
        copy.start()
    batches = gathered_ref.shape[0] // strips
    packs = sproj_ref.shape[0] // LANES
    told = gathered_ref[...].reshape((batches, strips) + gathered_ref.shape[1:])
    heard = told[:, 0]
    for i in range(1, strips):
        heard = heard + told[:, i]
    heard = heard.astype(BF).astype(F32)

    def column(p):
        return jnp.concatenate([heard[i, p : p + 1] for i in range(batches)], axis=0)

    state_pool = jnp.concatenate([column(p) for p in range(packs)], axis=1).astype(BF)
    goal_pool = jnp.concatenate([column(packs + p) for p in range(packs)], axis=1).astype(BF)
    index = jnp.concatenate([marks_ref[i] for i in range(batches)], axis=0)[:, 0:1]
    sharpness = marks_ref[batches][:, 0:1]
    state_unit, state_inverse = unit_of(dot(state_pool, sproj_ref[...], (1, 0)))
    goal_unit, goal_inverse = unit_of(dot(goal_pool, gproj_ref[...], (1, 0)))
    state_bf = state_unit.astype(BF)
    goal_bf = goal_unit.astype(BF)
    logits = sharpness * dot(state_bf, goal_bf, (1, 1))
    exp_logits = jnp.exp(logits)
    row_total = jnp.sum(exp_logits, axis=1, keepdims=True)
    matched = lax.broadcasted_iota(jnp.int32, logits.shape, 1).astype(F32) == index
    positive = jnp.sum(jnp.where(matched, logits, 0.0), axis=1, keepdims=True)
    losses = jnp.log(row_total) - positive
    mine = lax.broadcasted_iota(jnp.int32, losses.shape, 0) == lax.axis_index("batch")
    loss[0] = jnp.sum(jnp.where(mine, losses, 0.0))
    copies.append(pltpu.make_async_copy(loss, loss_ref, sem.at[len(copies)]))
    copies[-1].start()
    logit_grad = (exp_logits / row_total - matched.astype(F32)).astype(BF)
    for pool, unit, inverse, unit_grad, grad, target in (
        (state_pool, state_unit, state_inverse, dot(logit_grad, goal_bf, (1, 0)), sgrad, sgrad_ref),
        (goal_pool, goal_unit, goal_inverse, dot(logit_grad, state_bf, (0, 0)), ggrad, ggrad_ref),
    ):
        unit_grad = sharpness * unit_grad
        along = jnp.sum(unit * unit_grad, axis=-1, keepdims=True)
        emb_grad = ((unit_grad - unit * along) * inverse).astype(BF)
        for p in range(packs):
            span = slice(LANES * p, LANES * (p + 1))
            grad[span] = dot(pool[:, span], emb_grad, (0, 0))
            copies.append(pltpu.make_async_copy(grad.at[span], target.at[span], sem.at[len(copies)]))
            copies[-1].start()
    for copy in copies:
        copy.wait()


def shards(batches, strips, state_maps, goal_maps, conv_one, conv_two, state_proj, goal_proj, inv_temp, pair_index):
    _, rows, columns, channels = state_maps.shape
    width = state_proj.shape[1]
    taps_in = conv_one.shape[0] * conv_one.shape[1] * channels
    any_spec = pl.BlockSpec(memory_space=pl.ANY)
    vmem = pl.BlockSpec(memory_space=pltpu.VMEM)
    packs = channels // LANES
    dma = pltpu.SemaphoreType.DMA
    lines = 2 * packs
    stay = [
        pltpu.with_memory_space_constraint(value, pltpu.HBM)
        for value in (
            state_maps, goal_maps,
            conv_one.reshape(taps_in, channels), conv_two.reshape(taps_in, channels),
            state_proj, goal_proj,
        )
    ]
    held = pl.pallas_call(
        functools.partial(block_kernel, batches, strips),
        out_shape=(
            pltpu.VMEM((2, rows, packs, columns, LANES), F32),
            pltpu.VMEM((batches * strips, lines, LANES), F32),
            pltpu.VMEM((batches + 1, 1, LANES), F32),
            pltpu.VMEM((channels, width), BF),
            pltpu.VMEM((channels, width), BF),
        ),
        in_specs=[any_spec] * 8,
        out_specs=(vmem,) * 5,
        scratch_shapes=[
            pltpu.VMEM((2, rows, columns, channels), BF),
            pltpu.VMEM((2, rows + 4, packs, columns + 2 * PAD, LANES), F32),
            pltpu.VMEM((4, 2, rows + 4, columns // 2, channels), BF),
            pltpu.VMEM((4, 2, rows + 2, columns // 2, channels), BF),
            pltpu.VMEM((taps_in, channels), BF),
            pltpu.VMEM((taps_in, channels), BF),
            pltpu.VMEM((2, taps_in // 3, channels), BF),
            pltpu.VMEM((2, taps_in // 3, channels), BF),
            pltpu.VMEM((2, 2, 2, columns, channels), BF),
            pltpu.SMEM((1,), jnp.int32),
            pltpu.SMEM((1,), F32),
            pltpu.VMEM((1, LANES), F32),
            pltpu.VMEM((batches, 1, LANES), F32),
            pltpu.VMEM((lines, LANES), F32),
            pltpu.VMEM((batches * strips, lines, LANES), F32),
            dma((8,)), dma((2,)), dma((2,)), dma(()), dma(()), dma(()), dma(()),
        ],
        compiler_params=pltpu.CompilerParams(
            collective_id=0, has_side_effects=True, vmem_limit_bytes=40 * 2**20
        ),
        name="block",
    )(*stay, pair_index, inv_temp)
    held = [pltpu.with_memory_space_constraint(value, pltpu.VMEM) for value in held]
    return pl.pallas_call(
        functools.partial(head_kernel, strips),
        out_shape=(
            jax.ShapeDtypeStruct((1,), F32),
            jax.ShapeDtypeStruct((channels, width), F32),
            jax.ShapeDtypeStruct((channels, width), F32),
            jax.ShapeDtypeStruct((2, 1, rows, columns, channels), F32),
        ),
        in_specs=[vmem] * 5,
        out_specs=(any_spec,) * 4,
        scratch_shapes=[
            pltpu.SMEM((1,), F32),
            pltpu.VMEM((channels, width), F32),
            pltpu.VMEM((channels, width), F32),
            dma((1 + 3 * (channels // LANES),)),
        ],
        compiler_params=pltpu.CompilerParams(vmem_limit_bytes=40 * 2**20),
        name="head",
    )(*held)


def solution(mesh):
    placed = (
        P("batch", "strip", None, None),
        P("batch", "strip", None, None),
        P(),
        P(),
        P(),
        P(),
        P(),
        P("batch"),
    )
    return jax.shard_map(
        functools.partial(shards, mesh.shape["batch"], mesh.shape["strip"]),
        mesh=mesh,
        in_specs=placed,
        out_specs=(P("batch"), P(), P(), P(None, "batch", "strip", None, None)),
        check_vma=False,
    )
```

```python
import functools

import jax
import jax.numpy as jnp
from jax import lax
from jax.experimental import pallas as pl
from jax.experimental.pallas import tpu as pltpu
from jax.sharding import PartitionSpec as P

MESH = pl.DeviceIdType.MESH
BF = jnp.bfloat16
F32 = jnp.float32
LANES = 128
PAD = 8


def taps(store, k, frame, row, rows):
    pairs, channels = store.shape[3], store.shape[4]
    return jnp.concatenate(
        [store[k, frame, row + d : row + d + rows].reshape(rows * pairs, channels) for d in range(3)],
        axis=1,
    )


def stage(raw, frame, row, cells):
    columns = cells.shape[1]
    cells = cells.astype(F32)
    for h in range(raw.shape[2]):
        raw[frame, row : row + cells.shape[0], h, PAD : PAD + columns] = cells[:, :, LANES * h : LANES * (h + 1)]


def halved(raw, frame, row, first):
    pairs = (raw.shape[3] - 2 * PAD) // 2
    return [raw[frame, row, h, pl.ds(PAD + first, pairs, stride=2)] for h in range(raw.shape[2])]


def widen(store, raw, frame, rows):
    for row in rows:
        parts = [[jnp.maximum(x, 0.0) for x in halved(raw, frame, row, first)] for first in (-1, 0, 1, 2)]
        for h, (before, even, odd, after) in enumerate(zip(*parts)):
            lanes = slice(LANES * h, LANES * (h + 1))
            for k, value in enumerate((before - odd, even + odd, odd - even, even - after)):
                store[k, frame, row, :, lanes] = value.astype(BF)


def spread(store, frame, row, even, odd):
    rows, pairs, _ = even.shape
    where = lax.broadcasted_iota(jnp.int32, even.shape, 1)
    before = jnp.where(where == 0, 0.0, pltpu.roll(odd, 1, axis=1))
    after = jnp.where(where == pairs - 1, 0.0, pltpu.roll(even, pairs - 1, axis=1))
    span = slice(row, row + rows)
    for k, value in enumerate((before - odd, even + odd, odd - even, even - after)):
        store[k, frame, span] = value.astype(BF)


def mix(mixed, w):
    channels = w.shape[1]
    for d in range(3):
        left, centre, right = (
            w[(3 * d + c) * channels : (3 * d + c + 1) * channels].astype(F32) for c in range(3)
        )
        outer, inner = 0.5 * (left + right), 0.5 * centre
        span = slice(d * channels, (d + 1) * channels)
        mixed[0, span] = (outer + inner).astype(BF)
        mixed[1, span] = (outer - inner).astype(BF)


def products(store, w, mixed, pieces):
    channels = w.shape[1]
    out = [None] * 4
    for k in (0, 3, 1, 2):
        lhs = [taps(store, k, f, r, count) for f, r, count in pieces]
        lhs = lhs[0] if len(lhs) == 1 else jnp.concatenate(lhs, axis=0)
        if k in (0, 3):
            c = 0 if k == 0 else 2
            rhs = jnp.concatenate(
                [w[(3 * d + c) * channels : (3 * d + c + 1) * channels] for d in range(3)], axis=0
            )
        else:
            rhs = mixed[k - 1]
        out[k] = jnp.dot(lhs, rhs, preferred_element_type=F32)
    return out


def combine(out):
    return (out[1] + out[2]) + out[0], (out[1] - out[2]) - out[3]


def block_kernel(
    batches, strips,
    state_ref, goal_ref, one_ref, two_ref, sproj_ref, gproj_ref, index_ref, temp_ref,
    block_ref, gathered_ref, temp_out, sproj_out, gproj_out,
    maps, raw, wide_one, wide_two, w_one, w_two, mixed_one, mixed_two, halo, index, temp, part, parts,
    load_sem, halo_send, halo_recv, part_send, part_recv,
):
    b = lax.axis_index("batch")
    s = lax.axis_index("strip")
    rows, columns, channels = maps.shape[1], maps.shape[2], maps.shape[3]
    packs = channels // LANES
    devices = batches * strips
    me = b * strips + s

    loads = [
        pltpu.make_async_copy(source, target, load_sem.at[i])
        for i, (source, target) in enumerate((
            (state_ref.at[0], maps.at[0]),
            (goal_ref.at[0], maps.at[1]),
            (one_ref, w_one),
            (two_ref, w_two),
            (sproj_ref, sproj_out),
            (gproj_ref, gproj_out),
            (index_ref, index),
            (temp_ref, temp),
        ))
    ]
    for copy in loads:
        copy.start()

    @pl.when(s == 0)
    def _():
        halo[0] = jnp.zeros(halo.shape[1:], BF)

    @pl.when(s == strips - 1)
    def _():
        halo[1] = jnp.zeros(halo.shape[1:], BF)

    barrier = pltpu.get_barrier_semaphore()

    def greet(k, carry):
        other = lax.rem(b + k, batches)
        for t in range(strips):
            pl.semaphore_signal(barrier, inc=1, device_id=(other, t), device_id_type=MESH)
        return carry

    for t in range(1, strips):
        pl.semaphore_signal(barrier, inc=1, device_id=(b, lax.rem(s + t, strips)), device_id_type=MESH)
    lax.fori_loop(1, batches, greet, 0)
    edge = jnp.zeros((raw.shape[1], raw.shape[2], PAD, LANES), F32)
    for f in range(2):
        raw[f, :, :, 0:PAD] = edge
        raw[f, :, :, PAD + columns :] = edge

    down = pltpu.make_async_remote_copy(
        src_ref=maps.at[:, rows - 2 : rows], dst_ref=halo.at[0],
        send_sem=halo_send.at[0], recv_sem=halo_recv.at[0],
        device_id=(b, lax.rem(s + 1, strips)), device_id_type=MESH,
    )
    up = pltpu.make_async_remote_copy(
        src_ref=maps.at[:, 0:2], dst_ref=halo.at[1],
        send_sem=halo_send.at[1], recv_sem=halo_recv.at[1],
        device_id=(b, lax.rem(s + strips - 1, strips)), device_id_type=MESH,
    )

    def settle(buffer, sem, count):
        if count:
            pltpu.make_async_copy(buffer.at[0:count], buffer.at[0:count], sem).wait()

    above = jnp.where(s > 0, 1.0, 0.0)
    below = jnp.where(s < strips - 1, 1.0, 0.0)
    pairs = columns // 2
    inner = range(2, rows + 2)
    outer = (0, 1, rows + 2, rows + 3)
    totals = [[jnp.zeros((pairs, LANES), F32) for h in range(packs)] for f in range(2)]

    def first(pieces):
        return products(wide_one, w_one, mixed_one, [(f, r + 1, count) for f, r, count in pieces])

    def after_first(pieces, out):
        evens, odds = combine(out)
        at = 0
        for f, r, count in pieces:
            both = []
            for out in (evens, odds):
                piece = jnp.maximum(out[at : at + count * pairs], 0.0).reshape(count, pairs, channels)
                if r < 0:
                    piece = jnp.concatenate([piece[0:1] * above, piece[1:]], axis=0)
                if r + count > rows:
                    piece = jnp.concatenate([piece[: count - 1], piece[count - 1 :] * below], axis=0)
                both.append(piece)
            at += count * pairs
            spread(wide_two, f, r + 1, *both)

    def second(pieces):
        return products(wide_two, w_two, mixed_two, pieces)

    def after_second(pieces, out):
        evens, odds = combine(out)
        at = 0
        for f, r, count in pieces:
            for first, out in enumerate((evens, odds)):
                piece = out[at : at + count * pairs]
                for i in range(count):
                    skips = halved(raw, f, r + 2 + i, first)
                    for h, skip in enumerate(skips):
                        lanes = slice(LANES * h, LANES * (h + 1))
                        value = jnp.maximum(skip + piece[i * pairs : (i + 1) * pairs, lanes], 0.0)
                        block_ref[f, r + i, h, pl.ds(first, pairs, stride=2)] = value
                        totals[f][h] = totals[f][h] + value
            at += count * pairs

    loads[0].wait()
    stage(raw, 0, 2, maps[0])
    loads[1].wait()
    pl.semaphore_wait(barrier, devices - 1)

    @pl.when(s < strips - 1)
    def _():
        down.start()

    @pl.when(s > 0)
    def _():
        up.start()

    widen(wide_one, raw, 0, inner)
    loads[2].wait()
    mix(mixed_one, w_one)
    work = [
        [(0, 1, rows - 2)],
        [(0, -1, 2), (0, rows - 1, 2), (1, -1, rows // 2)],
        [(1, rows // 2 - 1, rows + 2 - rows // 2)],
    ]
    done_0 = first(work[0])
    stage(raw, 1, 2, maps[1])
    widen(wide_one, raw, 1, inner)

    @pl.when(s < strips - 1)
    def _():
        down.wait_send()
        up.wait_recv()

    @pl.when(s > 0)
    def _():
        up.wait_send()
        down.wait_recv()

    loads[3].wait()
    for f in range(2):
        stage(raw, f, 0, halo[0, f])
        stage(raw, f, rows + 2, halo[1, f])
        widen(wide_one, raw, f, outer)
    done_1 = first(work[1])
    after_first(work[0], done_0)
    mix(mixed_two, w_two)
    done_2 = first(work[2])
    after_first(work[1], done_1)
    half = rows // 2
    steps = [[(f, r, count)] for f in range(2) for r, count in ((0, half), (half, rows - half))]
    out = second(steps[0])
    after_first(work[2], done_2)
    for step, later in zip(steps, steps[1:]):
        following = second(later)
        after_second(step, out)
        out = following
    after_second(steps[-1], out)
    cells = rows * strips * columns
    lines = [jnp.sum(total, axis=0, keepdims=True) / cells for frame in totals for total in frame]
    loads[6].wait()
    lines.append(jnp.full((1, LANES), index[0].astype(F32)))
    lines.append(jnp.zeros((part.shape[0] - len(lines), LANES), F32))
    share = jnp.concatenate(lines, axis=0).astype(BF)
    part[...] = share
    parts[me] = share
    high = 2 * me // devices
    stride = devices - 1 - (devices - 2) * high
    nearest = (devices - 1) * (1 - high)

    def send(k, carry):
        other = lax.rem(nearest + k * stride, devices)

        @pl.when(other != me)
        def _():
            pltpu.make_async_remote_copy(
                src_ref=part, dst_ref=parts.at[me], send_sem=part_send, recv_sem=part_recv,
                device_id=(other // strips, lax.rem(other, strips)), device_id_type=MESH,
            ).start()

        return carry

    lax.fori_loop(0, devices, send, 0)
    for i in (4, 5, 7):
        loads[i].wait()
    temp_out[...] = jnp.full(temp_out.shape, temp[0])
    settle(parts, part_recv, devices - 1)
    gathered_ref[...] = parts[...]
    settle(parts, part_send, devices - 1)


def unit_of(emb):
    inverse = lax.rsqrt(jnp.sum(emb * emb, axis=-1, keepdims=True) + 1e-06)
    return emb * inverse, inverse


def dot(left, right, over):
    return lax.dot_general(left, right, ((over[0:1], over[1:2]), ((), ())), preferred_element_type=F32)


def head_kernel(
    strips, block_ref, gathered_ref, temp_ref, sproj_ref, gproj_ref,
    loss_ref, sgrad_ref, ggrad_ref, out_ref,
    loss, sgrad, ggrad, sem,
):
    copies = [
        pltpu.make_async_copy(
            block_ref.at[:, :, h], out_ref.at[:, 0, :, :, LANES * h : LANES * (h + 1)], sem.at[h]
        )
        for h in range(block_ref.shape[2])
    ]
    for copy in copies:
        copy.start()
    batches = gathered_ref.shape[0] // strips
    packs = sproj_ref.shape[0] // LANES
    told = gathered_ref[...].astype(F32).reshape((batches, strips) + gathered_ref.shape[1:])
    heard = told[:, 0]
    for i in range(1, strips):
        heard = heard + told[:, i]
    heard = heard.astype(BF).astype(F32)

    def column(p):
        return jnp.concatenate([heard[i, p : p + 1] for i in range(batches)], axis=0)

    state_pool = jnp.concatenate([column(p) for p in range(packs)], axis=1).astype(BF)
    goal_pool = jnp.concatenate([column(packs + p) for p in range(packs)], axis=1).astype(BF)
    index = jnp.concatenate([told[i, 0, 2 * packs : 2 * packs + 1] for i in range(batches)], axis=0)[:, 0:1]
    sharpness = temp_ref[0:1, 0:1]
    state_unit, state_inverse = unit_of(dot(state_pool, sproj_ref[...], (1, 0)))
    goal_unit, goal_inverse = unit_of(dot(goal_pool, gproj_ref[...], (1, 0)))
    state_bf = state_unit.astype(BF)
    goal_bf = goal_unit.astype(BF)
    logits = sharpness * dot(state_bf, goal_bf, (1, 1))
    exp_logits = jnp.exp(logits)
    row_total = jnp.sum(exp_logits, axis=1, keepdims=True)
    matched = lax.broadcasted_iota(jnp.int32, logits.shape, 1).astype(F32) == index
    positive = jnp.sum(jnp.where(matched, logits, 0.0), axis=1, keepdims=True)
    losses = jnp.log(row_total) - positive
    mine = lax.broadcasted_iota(jnp.int32, losses.shape, 0) == lax.axis_index("batch")
    loss[0] = jnp.sum(jnp.where(mine, losses, 0.0))
    copies.append(pltpu.make_async_copy(loss, loss_ref, sem.at[len(copies)]))
    copies[-1].start()
    logit_grad = (exp_logits / row_total - matched.astype(F32)).astype(BF)
    for pool, unit, inverse, unit_grad, grad, target in (
        (state_pool, state_unit, state_inverse, dot(logit_grad, goal_bf, (1, 0)), sgrad, sgrad_ref),
        (goal_pool, goal_unit, goal_inverse, dot(logit_grad, state_bf, (0, 0)), ggrad, ggrad_ref),
    ):
        unit_grad = sharpness * unit_grad
        along = jnp.sum(unit * unit_grad, axis=-1, keepdims=True)
        emb_grad = ((unit_grad - unit * along) * inverse).astype(BF)
        for p in range(packs):
            span = slice(LANES * p, LANES * (p + 1))
            grad[span] = dot(pool[:, span], emb_grad, (0, 0))
            copies.append(pltpu.make_async_copy(grad.at[span], target.at[span], sem.at[len(copies)]))
            copies[-1].start()
    for copy in copies:
        copy.wait()


def shards(batches, strips, state_maps, goal_maps, conv_one, conv_two, state_proj, goal_proj, inv_temp, pair_index):
    _, rows, columns, channels = state_maps.shape
    width = state_proj.shape[1]
    taps_in = conv_one.shape[0] * conv_one.shape[1] * channels
    any_spec = pl.BlockSpec(memory_space=pl.ANY)
    vmem = pl.BlockSpec(memory_space=pltpu.VMEM)
    packs = channels // LANES
    dma = pltpu.SemaphoreType.DMA
    lines = 8 * pl.cdiv(2 * packs + 1, 8)
    stay = [
        pltpu.with_memory_space_constraint(value, pltpu.HBM)
        for value in (
            state_maps, goal_maps,
            conv_one.reshape(taps_in, channels), conv_two.reshape(taps_in, channels),
            state_proj, goal_proj,
        )
    ]
    held = pl.pallas_call(
        functools.partial(block_kernel, batches, strips),
        out_shape=(
            pltpu.VMEM((2, rows, packs, columns, LANES), F32),
            pltpu.VMEM((batches * strips, lines, LANES), BF),
            pltpu.VMEM((8, LANES), F32),
            pltpu.VMEM((channels, width), BF),
            pltpu.VMEM((channels, width), BF),
        ),
        in_specs=[any_spec] * 8,
        out_specs=(vmem,) * 5,
        scratch_shapes=[
            pltpu.VMEM((2, rows, columns, channels), BF),
            pltpu.VMEM((2, rows + 4, packs, columns + 2 * PAD, LANES), F32),
            pltpu.VMEM((4, 2, rows + 4, columns // 2, channels), BF),
            pltpu.VMEM((4, 2, rows + 2, columns // 2, channels), BF),
            pltpu.VMEM((taps_in, channels), BF),
            pltpu.VMEM((taps_in, channels), BF),
            pltpu.VMEM((2, taps_in // 3, channels), BF),
            pltpu.VMEM((2, taps_in // 3, channels), BF),
            pltpu.VMEM((2, 2, 2, columns, channels), BF),
            pltpu.SMEM((1,), jnp.int32),
            pltpu.SMEM((1,), F32),
            pltpu.VMEM((lines, LANES), BF),
            pltpu.VMEM((batches * strips, lines, LANES), BF),
            dma((8,)), dma((2,)), dma((2,)), dma(()), dma(()),
        ],
        compiler_params=pltpu.CompilerParams(
            collective_id=0, has_side_effects=True, vmem_limit_bytes=40 * 2**20
        ),
        name="block",
    )(*stay, pair_index, inv_temp)
    held = [pltpu.with_memory_space_constraint(value, pltpu.VMEM) for value in held]
    return pl.pallas_call(
        functools.partial(head_kernel, strips),
        out_shape=(
            jax.ShapeDtypeStruct((1,), F32),
            jax.ShapeDtypeStruct((channels, width), F32),
            jax.ShapeDtypeStruct((channels, width), F32),
            jax.ShapeDtypeStruct((2, 1, rows, columns, channels), F32),
        ),
        in_specs=[vmem] * 5,
        out_specs=(any_spec,) * 4,
        scratch_shapes=[
            pltpu.SMEM((1,), F32),
            pltpu.VMEM((channels, width), F32),
            pltpu.VMEM((channels, width), F32),
            dma((1 + 3 * (channels // LANES),)),
        ],
        compiler_params=pltpu.CompilerParams(vmem_limit_bytes=40 * 2**20),
        name="head",
    )(*held)


def solution(mesh):
    placed = (
        P("batch", "strip", None, None),
        P("batch", "strip", None, None),
        P(),
        P(),
        P(),
        P(),
        P(),
        P("batch"),
    )
    return jax.shard_map(
        functools.partial(shards, mesh.shape["batch"], mesh.shape["strip"]),
        mesh=mesh,
        in_specs=placed,
        out_specs=(P("batch"), P(), P(), P(None, "batch", "strip", None, None)),
        check_vma=False,
    )
```

```python
import functools

import jax
import jax.numpy as jnp
from jax import lax
from jax.experimental import pallas as pl
from jax.experimental.pallas import tpu as pltpu
from jax.sharding import PartitionSpec as P

MESH = pl.DeviceIdType.MESH
BF = jnp.bfloat16
F32 = jnp.float32
LANES = 128
PAD = 8


def taps(store, k, frame, row, rows):
    pairs, channels = store.shape[3], store.shape[4]
    return jnp.concatenate(
        [store[k, frame, row + d : row + d + rows].reshape(rows * pairs, channels) for d in range(3)],
        axis=1,
    )


def stage(raw, frame, row, cells):
    columns = cells.shape[1]
    cells = cells.astype(F32)
    for h in range(raw.shape[2]):
        raw[frame, row : row + cells.shape[0], h, PAD : PAD + columns] = cells[:, :, LANES * h : LANES * (h + 1)]


def halved(raw, frame, row, first):
    pairs = (raw.shape[3] - 2 * PAD) // 2
    return [raw[frame, row, h, pl.ds(PAD + first, pairs, stride=2)] for h in range(raw.shape[2])]


def widen(store, raw, frame, rows):
    for row in rows:
        parts = [[jnp.maximum(x, 0.0) for x in halved(raw, frame, row, first)] for first in (-1, 0, 1, 2)]
        for h, (before, even, odd, after) in enumerate(zip(*parts)):
            lanes = slice(LANES * h, LANES * (h + 1))
            for k, value in enumerate((before - odd, even + odd, odd - even, even - after)):
                store[k, frame, row, :, lanes] = value.astype(BF)


def spread(store, frame, row, even, odd):
    rows, pairs, _ = even.shape
    where = lax.broadcasted_iota(jnp.int32, even.shape, 1)
    before = jnp.where(where == 0, 0.0, pltpu.roll(odd, 1, axis=1))
    after = jnp.where(where == pairs - 1, 0.0, pltpu.roll(even, pairs - 1, axis=1))
    span = slice(row, row + rows)
    for k, value in enumerate((before - odd, even + odd, odd - even, even - after)):
        store[k, frame, span] = value.astype(BF)


def mix(mixed, w):
    channels = w.shape[1]
    for d in range(3):
        left, centre, right = (
            w[(3 * d + c) * channels : (3 * d + c + 1) * channels].astype(F32) for c in range(3)
        )
        outer, inner = 0.5 * (left + right), 0.5 * centre
        span = slice(d * channels, (d + 1) * channels)
        mixed[0, span] = (outer + inner).astype(BF)
        mixed[1, span] = (outer - inner).astype(BF)


def products(store, w, mixed, pieces):
    channels = w.shape[1]
    out = [None] * 4
    for k in (0, 3, 1, 2):
        lhs = [taps(store, k, f, r, count) for f, r, count in pieces]
        lhs = lhs[0] if len(lhs) == 1 else jnp.concatenate(lhs, axis=0)
        if k in (0, 3):
            c = 0 if k == 0 else 2
            rhs = jnp.concatenate(
                [w[(3 * d + c) * channels : (3 * d + c + 1) * channels] for d in range(3)], axis=0
            )
        else:
            rhs = mixed[k - 1]
        out[k] = jnp.dot(lhs, rhs, preferred_element_type=F32)
    return out


def combine(out):
    return (out[1] + out[2]) + out[0], (out[1] - out[2]) - out[3]


def block_kernel(
    batches, strips,
    state_ref, goal_ref, one_ref, two_ref, sproj_ref, gproj_ref, index_ref, temp_ref,
    block_ref, gathered_ref, temp_out, sproj_out, gproj_out,
    maps, raw, wide_one, wide_two, w_one, w_two, mixed_one, mixed_two, halo, index, temp, part, parts,
    load_sem, halo_send, halo_recv, part_send, part_recv,
):
    b = lax.axis_index("batch")
    s = lax.axis_index("strip")
    rows, columns, channels = maps.shape[1], maps.shape[2], maps.shape[3]
    packs = channels // LANES
    devices = batches * strips
    me = b * strips + s

    loads = [
        pltpu.make_async_copy(source, target, load_sem.at[i])
        for i, (source, target) in enumerate((
            (state_ref.at[0], maps.at[0]),
            (goal_ref.at[0], maps.at[1]),
            (one_ref, w_one),
            (two_ref, w_two),
            (sproj_ref, sproj_out),
            (gproj_ref, gproj_out),
            (index_ref, index),
            (temp_ref, temp),
        ))
    ]
    for copy in loads:
        copy.start()

    @pl.when(s == 0)
    def _():
        halo[0] = jnp.zeros(halo.shape[1:], BF)

    @pl.when(s == strips - 1)
    def _():
        halo[1] = jnp.zeros(halo.shape[1:], BF)

    barrier = pltpu.get_barrier_semaphore()

    def greet(k, carry):
        other = lax.rem(b + k, batches)
        for t in range(strips):
            pl.semaphore_signal(barrier, inc=1, device_id=(other, t), device_id_type=MESH)
        return carry

    for t in range(1, strips):
        pl.semaphore_signal(barrier, inc=1, device_id=(b, lax.rem(s + t, strips)), device_id_type=MESH)
    lax.fori_loop(1, batches, greet, 0)
    edge = jnp.zeros((raw.shape[1], raw.shape[2], PAD, LANES), F32)
    for f in range(2):
        raw[f, :, :, 0:PAD] = edge
        raw[f, :, :, PAD + columns :] = edge

    down = pltpu.make_async_remote_copy(
        src_ref=maps.at[:, rows - 2 : rows], dst_ref=halo.at[0],
        send_sem=halo_send.at[0], recv_sem=halo_recv.at[0],
        device_id=(b, lax.rem(s + 1, strips)), device_id_type=MESH,
    )
    up = pltpu.make_async_remote_copy(
        src_ref=maps.at[:, 0:2], dst_ref=halo.at[1],
        send_sem=halo_send.at[1], recv_sem=halo_recv.at[1],
        device_id=(b, lax.rem(s + strips - 1, strips)), device_id_type=MESH,
    )

    def settle(buffer, sem, count):
        if count:
            pltpu.make_async_copy(buffer.at[0:count], buffer.at[0:count], sem).wait()

    above = jnp.where(s > 0, 1.0, 0.0)
    below = jnp.where(s < strips - 1, 1.0, 0.0)
    pairs = columns // 2
    inner = range(2, rows + 2)
    outer = (0, 1, rows + 2, rows + 3)
    totals = [[jnp.zeros((pairs, LANES), F32) for h in range(packs)] for f in range(2)]

    def first(pieces):
        return products(wide_one, w_one, mixed_one, [(f, r + 1, count) for f, r, count in pieces])

    def after_first(pieces, out):
        evens, odds = combine(out)
        at = 0
        for f, r, count in pieces:
            both = []
            for out in (evens, odds):
                piece = jnp.maximum(out[at : at + count * pairs], 0.0).reshape(count, pairs, channels)
                if r < 0:
                    piece = jnp.concatenate([piece[0:1] * above, piece[1:]], axis=0)
                if r + count > rows:
                    piece = jnp.concatenate([piece[: count - 1], piece[count - 1 :] * below], axis=0)
                both.append(piece)
            at += count * pairs
            spread(wide_two, f, r + 1, *both)

    def second(pieces):
        return products(wide_two, w_two, mixed_two, pieces)

    def after_second(pieces, out):
        evens, odds = combine(out)
        at = 0
        for f, r, count in pieces:
            for first, out in enumerate((evens, odds)):
                piece = out[at : at + count * pairs]
                for i in range(count):
                    skips = halved(raw, f, r + 2 + i, first)
                    for h, skip in enumerate(skips):
                        lanes = slice(LANES * h, LANES * (h + 1))
                        value = jnp.maximum(skip + piece[i * pairs : (i + 1) * pairs, lanes], 0.0)
                        block_ref[f, r + i, h, pl.ds(first, pairs, stride=2)] = value
                        totals[f][h] = totals[f][h] + value
            at += count * pairs

    loads[0].wait()
    stage(raw, 0, 2, maps[0])
    loads[1].wait()
    pl.semaphore_wait(barrier, devices - 1)

    @pl.when(s < strips - 1)
    def _():
        down.start()

    @pl.when(s > 0)
    def _():
        up.start()

    widen(wide_one, raw, 0, inner)
    loads[2].wait()
    mix(mixed_one, w_one)
    work = [
        [(0, 1, rows - 2)],
        [(0, -1, 2), (0, rows - 1, 2), (1, -1, rows // 2)],
        [(1, rows // 2 - 1, rows + 2 - rows // 2)],
    ]
    done_0 = first(work[0])
    stage(raw, 1, 2, maps[1])
    widen(wide_one, raw, 1, inner)

    @pl.when(s < strips - 1)
    def _():
        down.wait_send()
        up.wait_recv()

    @pl.when(s > 0)
    def _():
        up.wait_send()
        down.wait_recv()

    loads[3].wait()
    for f in range(2):
        stage(raw, f, 0, halo[0, f])
        stage(raw, f, rows + 2, halo[1, f])
        widen(wide_one, raw, f, outer)
    done_1 = first(work[1])
    after_first(work[0], done_0)
    mix(mixed_two, w_two)
    done_2 = first(work[2])
    after_first(work[1], done_1)
    half = rows // 2
    steps = [[(f, r, count)] for f in range(2) for r, count in ((0, half), (half, rows - half))]
    out = second(steps[0])
    after_first(work[2], done_2)
    for step, later in zip(steps, steps[1:]):
        following = second(later)
        after_second(step, out)
        out = following
    after_second(steps[-1], out)
    cells = rows * strips * columns
    lines = [jnp.sum(total, axis=0, keepdims=True) / cells for frame in totals for total in frame]
    loads[6].wait()
    lines.append(jnp.full((1, LANES), index[0].astype(F32)))
    lines.append(jnp.zeros((part.shape[0] - len(lines), LANES), F32))
    share = jnp.concatenate(lines, axis=0).astype(BF)
    part[...] = share
    parts[me] = share
    high = 2 * b // batches
    way = batches - 1 - (batches - 2) * high
    first_peer = (batches - 1) * (1 - high)

    def send(other, t):
        pltpu.make_async_remote_copy(
            src_ref=part, dst_ref=parts.at[me], send_sem=part_send, recv_sem=part_recv,
            device_id=(other, t), device_id_type=MESH,
        ).start()

    def spray(k, carry):
        other = lax.rem(first_peer + k * way, batches)

        @pl.when(other != b)
        def _():
            for t in range(strips):
                send(other, t)

        return carry

    lax.fori_loop(0, batches, spray, 0)
    for t in range(1, strips):
        send(b, lax.rem(s + t, strips))
    for i in (4, 5, 7):
        loads[i].wait()
    temp_out[...] = jnp.full(temp_out.shape, temp[0])
    settle(parts, part_recv, devices - 1)
    gathered_ref[...] = parts[...]
    settle(parts, part_send, devices - 1)


def unit_of(emb):
    inverse = lax.rsqrt(jnp.sum(emb * emb, axis=-1, keepdims=True) + 1e-06)
    return emb * inverse, inverse


def dot(left, right, over):
    return lax.dot_general(left, right, ((over[0:1], over[1:2]), ((), ())), preferred_element_type=F32)


def head_kernel(
    strips, block_ref, gathered_ref, temp_ref, sproj_ref, gproj_ref,
    loss_ref, sgrad_ref, ggrad_ref, out_ref,
    loss, sgrad, ggrad, sem,
):
    copies = [
        pltpu.make_async_copy(
            block_ref.at[:, :, h], out_ref.at[:, 0, :, :, LANES * h : LANES * (h + 1)], sem.at[h]
        )
        for h in range(block_ref.shape[2])
    ]
    for copy in copies:
        copy.start()
    batches = gathered_ref.shape[0] // strips
    packs = sproj_ref.shape[0] // LANES
    told = gathered_ref[...].astype(F32).reshape((batches, strips) + gathered_ref.shape[1:])
    heard = told[:, 0]
    for i in range(1, strips):
        heard = heard + told[:, i]
    heard = heard.astype(BF).astype(F32)

    def column(p):
        return jnp.concatenate([heard[i, p : p + 1] for i in range(batches)], axis=0)

    state_pool = jnp.concatenate([column(p) for p in range(packs)], axis=1).astype(BF)
    goal_pool = jnp.concatenate([column(packs + p) for p in range(packs)], axis=1).astype(BF)
    index = jnp.concatenate([told[i, 0, 2 * packs : 2 * packs + 1] for i in range(batches)], axis=0)[:, 0:1]
    sharpness = temp_ref[0:1, 0:1]
    state_unit, state_inverse = unit_of(dot(state_pool, sproj_ref[...], (1, 0)))
    goal_unit, goal_inverse = unit_of(dot(goal_pool, gproj_ref[...], (1, 0)))
    state_bf = state_unit.astype(BF)
    goal_bf = goal_unit.astype(BF)
    logits = sharpness * dot(state_bf, goal_bf, (1, 1))
    exp_logits = jnp.exp(logits)
    row_total = jnp.sum(exp_logits, axis=1, keepdims=True)
    matched = lax.broadcasted_iota(jnp.int32, logits.shape, 1).astype(F32) == index
    positive = jnp.sum(jnp.where(matched, logits, 0.0), axis=1, keepdims=True)
    losses = jnp.log(row_total) - positive
    mine = lax.broadcasted_iota(jnp.int32, losses.shape, 0) == lax.axis_index("batch")
    loss[0] = jnp.sum(jnp.where(mine, losses, 0.0))
    copies.append(pltpu.make_async_copy(loss, loss_ref, sem.at[len(copies)]))
    copies[-1].start()
    logit_grad = (exp_logits / row_total - matched.astype(F32)).astype(BF)
    for pool, unit, inverse, unit_grad, grad, target in (
        (state_pool, state_unit, state_inverse, dot(logit_grad, goal_bf, (1, 0)), sgrad, sgrad_ref),
        (goal_pool, goal_unit, goal_inverse, dot(logit_grad, state_bf, (0, 0)), ggrad, ggrad_ref),
    ):
        unit_grad = sharpness * unit_grad
        along = jnp.sum(unit * unit_grad, axis=-1, keepdims=True)
        emb_grad = ((unit_grad - unit * along) * inverse).astype(BF)
        for p in range(packs):
            span = slice(LANES * p, LANES * (p + 1))
            grad[span] = dot(pool[:, span], emb_grad, (0, 0))
            copies.append(pltpu.make_async_copy(grad.at[span], target.at[span], sem.at[len(copies)]))
            copies[-1].start()
    for copy in copies:
        copy.wait()


def shards(batches, strips, state_maps, goal_maps, conv_one, conv_two, state_proj, goal_proj, inv_temp, pair_index):
    _, rows, columns, channels = state_maps.shape
    width = state_proj.shape[1]
    taps_in = conv_one.shape[0] * conv_one.shape[1] * channels
    any_spec = pl.BlockSpec(memory_space=pl.ANY)
    vmem = pl.BlockSpec(memory_space=pltpu.VMEM)
    packs = channels // LANES
    dma = pltpu.SemaphoreType.DMA
    lines = 8 * pl.cdiv(2 * packs + 1, 8)
    stay = [
        pltpu.with_memory_space_constraint(value, pltpu.HBM)
        for value in (
            state_maps, goal_maps,
            conv_one.reshape(taps_in, channels), conv_two.reshape(taps_in, channels),
            state_proj, goal_proj,
        )
    ]
    held = pl.pallas_call(
        functools.partial(block_kernel, batches, strips),
        out_shape=(
            pltpu.VMEM((2, rows, packs, columns, LANES), F32),
            pltpu.VMEM((batches * strips, lines, LANES), BF),
            pltpu.VMEM((8, LANES), F32),
            pltpu.VMEM((channels, width), BF),
            pltpu.VMEM((channels, width), BF),
        ),
        in_specs=[any_spec] * 8,
        out_specs=(vmem,) * 5,
        scratch_shapes=[
            pltpu.VMEM((2, rows, columns, channels), BF),
            pltpu.VMEM((2, rows + 4, packs, columns + 2 * PAD, LANES), F32),
            pltpu.VMEM((4, 2, rows + 4, columns // 2, channels), BF),
            pltpu.VMEM((4, 2, rows + 2, columns // 2, channels), BF),
            pltpu.VMEM((taps_in, channels), BF),
            pltpu.VMEM((taps_in, channels), BF),
            pltpu.VMEM((2, taps_in // 3, channels), BF),
            pltpu.VMEM((2, taps_in // 3, channels), BF),
            pltpu.VMEM((2, 2, 2, columns, channels), BF),
            pltpu.SMEM((1,), jnp.int32),
            pltpu.SMEM((1,), F32),
            pltpu.VMEM((lines, LANES), BF),
            pltpu.VMEM((batches * strips, lines, LANES), BF),
            dma((8,)), dma((2,)), dma((2,)), dma(()), dma(()),
        ],
        compiler_params=pltpu.CompilerParams(
            collective_id=0, has_side_effects=True, vmem_limit_bytes=40 * 2**20
        ),
        name="block",
    )(*stay, pair_index, inv_temp)
    held = [pltpu.with_memory_space_constraint(value, pltpu.VMEM) for value in held]
    return pl.pallas_call(
        functools.partial(head_kernel, strips),
        out_shape=(
            jax.ShapeDtypeStruct((1,), F32),
            jax.ShapeDtypeStruct((channels, width), F32),
            jax.ShapeDtypeStruct((channels, width), F32),
            jax.ShapeDtypeStruct((2, 1, rows, columns, channels), F32),
        ),
        in_specs=[vmem] * 5,
        out_specs=(any_spec,) * 4,
        scratch_shapes=[
            pltpu.SMEM((1,), F32),
            pltpu.VMEM((channels, width), F32),
            pltpu.VMEM((channels, width), F32),
            dma((1 + 3 * (channels // LANES),)),
        ],
        compiler_params=pltpu.CompilerParams(vmem_limit_bytes=40 * 2**20),
        name="head",
    )(*held)


def solution(mesh):
    placed = (
        P("batch", "strip", None, None),
        P("batch", "strip", None, None),
        P(),
        P(),
        P(),
        P(),
        P(),
        P("batch"),
    )
    return jax.shard_map(
        functools.partial(shards, mesh.shape["batch"], mesh.shape["strip"]),
        mesh=mesh,
        in_specs=placed,
        out_specs=(P("batch"), P(), P(), P(None, "batch", "strip", None, None)),
        check_vma=False,
    )
```
